32 devices in a mesh: tm: 8 (over z, y), tensor: 4 (over x, core).
Axes of the slice: x: 2, y: 2, z: 4, core: 2. Of those that a mesh axis runs over, the one named last changes fastest.
Arguments:
- frames_in: bfloat16 [8, 528, 1024], P('tm'), may hold values from -6 to 6
- frame_time: int32 [8], replicated, may hold values from 0 to 7, each once
- cond_count: int32 [8], replicated, may hold values from 0 to 2
- ln1_gain: float32 [2, 1024], replicated, may hold values from 0.5 to 1.5
- ln1_bias: float32 [2, 1024], replicated, may hold values from -1.75 to 1.75
- qkv_weight: bfloat16 [2, 3, 1024, 1024], P(None, None, None, 'tensor'), may hold values from -17 to 17
- qkv_bias: float32 [2, 3, 1024], P(None, None, 'tensor'), may hold values from -1.75 to 1.75
- out_weight: bfloat16 [2, 1024, 1024], P(None, 'tensor'), may hold values from -0.1875 to 0.1875
- out_bias: float32 [2, 1024], replicated, may hold values from -1.75 to 1.75
- ln2_gain: float32 [2, 1024], replicated, may hold values from 0.5 to 1.5
- ln2_bias: float32 [2, 1024], replicated, may hold values from -1.75 to 1.75
- fc1_weight: bfloat16 [2, 1024, 4096], P(None, None, 'tensor'), may hold values from -0.1875 to 0.1875
- fc1_bias: float32 [2, 4096], P(None, 'tensor'), may hold values from -3 to 3
- fc2_weight: bfloat16 [2, 4096, 1024], P(None, 'tensor'), may hold values from -0.09375 to 0.09375
- fc2_bias: float32 [2, 1024], replicated, may hold values from -1.75 to 1.75
Outputs:
- frames_out: bfloat16 [8, 528, 1024], P('tm', 'tensor')
The draws below stay inside these ranges and needn't reach their ends.
Inputs may be any that keep to these rules, and one draw needn't show every extreme that they name: `frame_time`: every time index 0 to 7 appears once. `cond_count`: the valid action and state tokens of a frame are its first ones.
All inputs are finite; a program needn't handle non-finite values.
Results may differ from the reference program's by a relative error of at most 0.04.
Values may be sent and summed in bfloat16 or wider, within the bound.
A program may use at most 128 MiB of HBM per device.

```python
import jax
import jax.numpy as jnp
from jax import lax

D = 1024
HEADS = 16
FF = 4096
PATCH_DEV = 64
COND = 2
SEQS = 8
LAYERS = 2
FRAMES = 8
ROWS = 528
N_TM = 8


def draw_qkv_weight(key, part):
    weights_raw = jnp.clip(jax.random.normal(jax.random.fold_in(key, 101), (LAYERS, 3, D, D), jnp.float32), -5.0, 5.0) * D ** (-0.5)
    return weights_raw.astype(jnp.bfloat16)


def plant(values, stream_key, low, high):
    longest = values.shape.index(max(values.shape))
    spots = []
    for shift in (0, 1):
        where = [jax.random.randint(jax.random.fold_in(stream_key, axis), (), 0, length) for axis, length in enumerate(values.shape)]
        where[longest] = (where[longest] + shift) % values.shape[longest]
        spots.append(tuple(where))
    return values.at[spots[0]].set(low).at[spots[1]].set(high)


def shard_levels(rng, shape, cuts, low, largest):
    gain, own = 1.0, jax.random.fold_in(rng, 6)
    for dim, parts in cuts:
        draws = jnp.exp(jax.random.uniform(jax.random.fold_in(own, dim), (parts,), jnp.float32, low / len(cuts), largest / len(cuts)))
        gain = gain * jnp.repeat(draws, shape[dim] // parts).reshape([-1 if axis == dim else 1 for axis in range(len(shape))])
    return gain


def normal_values(rng, dims, scale, limit, split=(), kind=jnp.bfloat16):
    array = jax.random.normal(rng, dims, jnp.float32) * scale
    if len(split) > 0:
        array = shard_levels(rng, dims, split, -0.22, 0.18) * array
    return jnp.clip(array, min=-limit, max=limit).astype(kind)


def setup_inputs(seed: int = 0) -> dict:
    keys = jax.random.split(jax.random.key(seed), 16)
    return {
        "frames_in": normal_values(keys[0], (N_TM, ROWS, D), 1.0, 6.0, ((0, 8),)),
        "frame_time": jax.random.permutation(keys[1], FRAMES).astype(jnp.int32),
        "cond_count": plant(jax.random.randint(keys[2], (FRAMES,), 0, COND + 1), jax.random.fold_in(keys[2], 1), 0, COND).astype(jnp.int32),
        "ln1_gain": jnp.clip(1.0 + 0.1 * jax.random.normal(keys[3], (LAYERS, D), jnp.float32), 0.5, 1.5),
        "ln1_bias": normal_values(keys[4], (LAYERS, D), 0.3, 1.75, (), jnp.float32),
        "qkv_weight": draw_qkv_weight(jax.random.fold_in(keys[15], 71), 0),
        "qkv_bias": normal_values(keys[6], (LAYERS, 3, D), 0.3, 1.75, ((2, 4),), jnp.float32),
        "out_weight": normal_values(keys[7], (LAYERS, D, D), D ** -0.5, 0.1875, ((1, 4),)),
        "out_bias": normal_values(keys[8], (LAYERS, D), 0.3, 1.75, (), jnp.float32),
        "ln2_gain": jnp.clip(1.0 + 0.1 * jax.random.normal(keys[9], (LAYERS, D), jnp.float32), 0.5, 1.5),
        "ln2_bias": normal_values(keys[10], (LAYERS, D), 0.3, 1.75, (), jnp.float32),
        "fc1_weight": normal_values(keys[11], (LAYERS, D, FF), D ** -0.5, 0.1875, ((2, 4),)),
        "fc1_bias": normal_values(keys[12], (LAYERS, FF), 0.5, 3.0, ((1, 4),), jnp.float32),
        "fc2_weight": normal_values(keys[13], (LAYERS, FF, D), FF ** -0.5, 0.09375, ((1, 4),)),
        "fc2_bias": normal_values(keys[14], (LAYERS, D), 0.3, 1.75, (), jnp.float32),
    }


def layer_norm(inputs, gain_row, bias_row):
    center = lax.optimization_barrier(jnp.mean(inputs, axis=-1, keepdims=True))
    spread = lax.optimization_barrier(jnp.mean(jnp.square(inputs - center), axis=-1, keepdims=True))
    return (inputs - center) * lax.rsqrt(spread + 1e-06) * gain_row + bias_row

def piece_tables(frame_time, cond_count, piece_count, frame_split, piece_rows):
    cond_dev = COND // frame_split
    piece_ids = jnp.arange(piece_count, dtype=jnp.int32)
    frame_ids = jnp.arange(frame_time.shape[0], dtype=jnp.int32)
    matches = (piece_ids // frame_split)[:, None] == frame_ids[None, :]
    piece_time = lax.optimization_barrier(jnp.sum(jnp.where(matches, frame_time[None, :], 0), axis=1)).astype(jnp.int32)
    piece_cond = lax.optimization_barrier(jnp.sum(jnp.where(matches, cond_count[None, :], 0), axis=1)).astype(jnp.int32)
    slot_index = jnp.arange(piece_rows, dtype=jnp.int32)
    cond_slot = (piece_ids % frame_split)[:, None] * cond_dev + slot_index[None, :] - PATCH_DEV
    valid = (slot_index[None, :] < PATCH_DEV) | (cond_slot < piece_cond[:, None])
    return (piece_time, valid)

def reference(frames_in, frame_time, cond_count, ln1_gain, ln1_bias, qkv_weight, qkv_bias, out_weight, out_bias, ln2_gain, ln2_bias, fc1_weight, fc1_bias, fc2_weight, fc2_bias):
    frame_split = N_TM // FRAMES
    cond_dev = COND // frame_split
    piece_rows = PATCH_DEV + cond_dev
    piece_time, valid = piece_tables(frame_time, cond_count, N_TM, frame_split, piece_rows)
    head_dim = D // HEADS
    scale = head_dim ** (-0.5)
    stream = frames_in
    for layer_idx in range(LAYERS):
        flattened = stream.reshape(-1, D).astype(jnp.float32)
        normed = layer_norm(flattened, ln1_gain[layer_idx], ln1_bias[layer_idx]).astype(jnp.bfloat16)
        projected = []
        for part_idx in range(3):
            result = jnp.dot(normed, qkv_weight[layer_idx, part_idx], preferred_element_type=jnp.float32) + qkv_bias[layer_idx, part_idx]
            result = lax.optimization_barrier(result.astype(jnp.bfloat16))
            projected.append(result.astype(jnp.float32).reshape(N_TM, SEQS, piece_rows, HEADS, head_dim))
        queries, keys_all, values_all = projected

        def one_piece(piece_idx):
            query_block = lax.dynamic_index_in_dim(queries, piece_idx, 0, keepdims=False)
            scores = jnp.einsum('sqhd,gskhd->shqgk', query_block, keys_all) * scale
            my_time = lax.dynamic_index_in_dim(piece_time, piece_idx, 0, keepdims=False)
            allowed = (piece_time <= my_time)[:, None] & valid
            scores = jnp.where(allowed, scores, -1e+30)
            highest = lax.optimization_barrier(jnp.max(scores, axis=(3, 4), keepdims=True))
            weights = jnp.where(allowed, jnp.exp(scores - highest), 0.0)
            totals = lax.optimization_barrier(jnp.sum(weights, axis=(3, 4)))
            rounded = lax.optimization_barrier(weights.astype(jnp.bfloat16)).astype(jnp.float32)
            mixed = jnp.einsum('shqgk,gskhd->shqd', rounded, values_all) / totals[..., None]
            return jnp.transpose(mixed, (0, 2, 1, 3)).reshape(SEQS * piece_rows, D).astype(jnp.bfloat16)
        attended = lax.map(one_piece, jnp.arange(N_TM, dtype=jnp.int32))
        projection = jnp.dot(attended.reshape(-1, D), out_weight[layer_idx], preferred_element_type=jnp.float32)
        first = flattened + projection + out_bias[layer_idx]
        normed_two = layer_norm(first, ln2_gain[layer_idx], ln2_bias[layer_idx]).astype(jnp.bfloat16)
        inner = jax.nn.gelu(jnp.dot(normed_two, fc1_weight[layer_idx], preferred_element_type=jnp.float32) + fc1_bias[layer_idx], approximate=False).astype(jnp.bfloat16)
        output = jnp.dot(inner, fc2_weight[layer_idx], preferred_element_type=jnp.float32)
        stream = (first + output + fc2_bias[layer_idx]).astype(jnp.bfloat16).reshape(N_TM, SEQS * piece_rows, D)
    return stream
```

```python
import jax
import jax.numpy as jnp
from jax import lax
from jax.experimental import pallas as pl
from jax.experimental.pallas import tpu as pltpu
from jax.sharding import PartitionSpec as P

D = 1024
HEADS = 16
PATCH_DEV = 64
COND = 2
LAYERS = 2


def layer_norm(inputs, gain_row, bias_row):
    center = jnp.mean(inputs, axis=-1, keepdims=True)
    spread = jnp.mean(jnp.square(inputs - center), axis=-1, keepdims=True)
    return (inputs - center) * lax.rsqrt(spread + 1e-06) * gain_row + bias_row


def piece_tables(frame_time, cond_count, piece_count, frame_split, piece_rows):
    cond_dev = COND // frame_split
    piece_ids = jnp.arange(piece_count, dtype=jnp.int32)
    frame_ids = jnp.arange(frame_time.shape[0], dtype=jnp.int32)
    matches = (piece_ids // frame_split)[:, None] == frame_ids[None, :]
    piece_time = jnp.sum(jnp.where(matches, frame_time[None, :], 0), axis=1)
    piece_cond = jnp.sum(jnp.where(matches, cond_count[None, :], 0), axis=1)
    slot_index = jnp.arange(piece_rows, dtype=jnp.int32)
    cond_slot = (piece_ids % frame_split)[:, None] * cond_dev + slot_index[None, :] - PATCH_DEV
    valid = (slot_index[None, :] < PATCH_DEV) | (cond_slot < piece_cond[:, None])
    return (piece_time, valid)


def shards_gather(
    frames_in,
    frame_time,
    cond_count,
    ln1_gain,
    ln1_bias,
    qkv_weight,
    qkv_bias,
    out_weight,
    out_bias,
    ln2_gain,
    ln2_bias,
    fc1_weight,
    fc1_bias,
    fc2_weight,
    fc2_bias,
):
    frame_count = frame_time.shape[0]
    piece_count = lax.axis_size("tm")
    frame_split = piece_count // frame_count
    cond_dev = COND // frame_split
    piece_rows = PATCH_DEV + cond_dev
    row_count = frames_in.shape[1]
    seq_count = row_count // piece_rows
    head_dim = D // HEADS
    head_local = qkv_weight.shape[3] // head_dim
    scale = head_dim ** (-0.5)
    tensor_size = lax.axis_size("tensor")
    tensor_pos = lax.axis_index("tensor")
    my_piece = lax.axis_index("tm")
    share_rows = row_count // tensor_size
    piece_time, valid = piece_tables(frame_time, cond_count, piece_count, frame_split, piece_rows)
    piece_ids = jnp.arange(piece_count, dtype=jnp.int32)
    my_time = jnp.sum(jnp.where(piece_ids == my_piece, piece_time, 0))
    full_in = frames_in[0]
    new_share = None
    for layer_idx in range(LAYERS):
        normed = layer_norm(
            full_in.astype(jnp.float32), ln1_gain[layer_idx], ln1_bias[layer_idx]
        ).astype(jnp.bfloat16)
        projected = jnp.einsum(
            "rd,jde->jre", normed, qkv_weight[layer_idx], preferred_element_type=jnp.float32
        )
        projected = (projected + qkv_bias[layer_idx][:, None, :]).astype(jnp.bfloat16)
        queries = projected[0].reshape(seq_count, piece_rows, head_local, head_dim)
        keys_mine = projected[1].reshape(1, seq_count, piece_rows, head_local * head_dim)
        values_mine = projected[2].reshape(1, seq_count, piece_rows, head_local * head_dim)
        start_top = jnp.full((seq_count, head_local, piece_rows), -1e30, jnp.float32)
        key_block = lax.all_gather(keys_mine, "tm", axis=0, tiled=True)
        value_block = lax.all_gather(values_mine, "tm", axis=0, tiled=True)
        block_count = key_block.shape[0]
        block_ids = jnp.arange(block_count, dtype=jnp.int32)
        matches = block_ids[:, None] == piece_ids[None, :]
        key_time = jnp.sum(jnp.where(matches, piece_time[None, :], 0), axis=1)
        key_valid = jnp.any(matches[:, :, None] & valid[None, :, :], axis=1)
        allowed = (key_time <= my_time)[:, None] & key_valid
        top_run = start_top
        keys_split = key_block.reshape(block_count, seq_count, piece_rows, head_local, head_dim)
        values_split = value_block.reshape(block_count, seq_count, piece_rows, head_local, head_dim)
        scores = (
            jnp.einsum("sqhd,gskhd->shqgk", queries, keys_split, preferred_element_type=jnp.float32)
            * scale
        )
        scores = jnp.where(allowed, scores, -1e30)
        new_top = jnp.maximum(top_run, jnp.max(scores, axis=(3, 4)))
        weights = jnp.where(allowed, jnp.exp(scores - new_top[..., None, None]), 0.0)
        total_new = jnp.sum(weights, axis=(3, 4))
        mixed = jnp.einsum(
            "shqgk,gskhd->shqd",
            weights.astype(jnp.bfloat16),
            values_split,
            preferred_element_type=jnp.float32,
        )
        top_run = new_top
        attended = (
            (mixed / total_new[..., None])
            .transpose(0, 2, 1, 3)
            .reshape(row_count, head_local * head_dim)
            .astype(jnp.bfloat16)
        )
        out_layer = out_weight[layer_idx]
        fc1_layer = fc1_weight[layer_idx]
        fc2_layer = fc2_weight[layer_idx]
        fc1_layer_bias = fc1_bias[layer_idx]
        own_rows = lax.dynamic_slice_in_dim(full_in, tensor_pos * share_rows, share_rows, 0).astype(
            jnp.float32
        )
        first = (
            own_rows
            + lax.psum_scatter(
                jnp.dot(attended, out_layer, preferred_element_type=jnp.float32).astype(
                    jnp.bfloat16
                ),
                "tensor",
                scatter_dimension=0,
                tiled=True,
            ).astype(jnp.float32)
            + out_bias[layer_idx]
        )
        normed_two = layer_norm(first, ln2_gain[layer_idx], ln2_bias[layer_idx]).astype(
            jnp.bfloat16
        )
        inner = jax.nn.gelu(
            jnp.dot(
                lax.all_gather(normed_two, "tensor", axis=0, tiled=True),
                fc1_layer,
                preferred_element_type=jnp.float32,
            )
            + fc1_layer_bias,
            approximate=False,
        ).astype(jnp.bfloat16)
        mlp_share = lax.psum_scatter(
            jnp.dot(inner, fc2_layer, preferred_element_type=jnp.float32).astype(jnp.bfloat16),
            "tensor",
            scatter_dimension=0,
            tiled=True,
        ).astype(jnp.float32)
        new_share = (first + mlp_share + fc2_bias[layer_idx]).astype(jnp.bfloat16)
        if layer_idx + 1 < LAYERS:
            full_in = lax.all_gather(new_share, "tensor", axis=0, tiled=True)
    return new_share[None]


MESH = pl.DeviceIdType.MESH
FAR = 1 << 30
N1, AP, AD, AO, N2, RP, XS = 0, 2, 4, 6, 8, 10, 12
IDS = 14
OWN, PIECE, REST, SPREAD = 0, 1, 2, 3


def clip_kernel(
    x_ref, time_ref, cond_ref, g1, b1, qkvb, ob, g2, b2, f1b, f2b, wqkv_h, wo_h, w1_h, w2_h,
    out_ref, wqkv, wo, w1, w2, blk_s, blk_r, xs, keep, nrm1, nrm2, qb, kb, vb, mask, att, att_p,
    inner, stg, rp, us, ur, out_s, out_r,
    wsem, in_s, in_r, fw_s, fw_r, loc, ls, lr, ws, wr, os, orr,
):
    groups = blk_s.shape[0]
    half = blk_r.shape[0]
    piece = blk_r.shape[1]
    patch = PATCH_DEV
    rows = xs.shape[0]
    lead = rows - half * patch
    cut = lead + (half // 2) * patch
    chunks = ((0, cut), (cut, rows - cut))
    head_dim = D // HEADS
    width = qb.shape[1]
    head_local = width // head_dim
    share = width // groups
    last = LAYERS - 1

    t = lax.axis_index("tm")
    me = lax.axis_index("tensor")
    x = me // 2
    c = me % 2
    partner = me + 1 - 2 * c
    across = (me + 2) % 4
    diagonal = (partner + 2) % 4

    def clip_of(g):
        return g // 2 + half * ((g // 2 + g) % 2)

    def group_of(clip):
        z = clip % half
        return 2 * z + (clip // half + z) % 2

    clip = clip_of(t)
    goal_x = clip // half
    goal = clip // 2

    pairs = ((wqkv_h, wqkv), (wo_h, wo), (w1_h, w1), (w2_h, w2))

    def weight_copy(l, j):
        dst = pairs[j][1].at[l]
        if j == 1:
            dst = wo.at[l, pl.ds(pl.multiple_of(me * width, width), width)]
        return pltpu.make_async_copy(pairs[j][0].at[l], dst, wsem.at[l, j])

    for l in range(LAYERS):
        for j in ((1, 0, 2, 3) if l == 0 else (0, 1, 2, 3)):
            weight_copy(l, j).start()

    def remote(src, dst, s, r, to):
        return pltpu.make_async_remote_copy(
            src_ref=src, dst_ref=dst, send_sem=s, recv_sem=r, device_id=to, device_id_type=MESH
        )

    barrier = pltpu.get_barrier_semaphore()

    def hello(g, j):
        pl.semaphore_signal(barrier, inc=1, device_id=(g, j), device_id_type=MESH)

    for other in (partner, across, diagonal):
        hello(t, other)
    for d in range(1, groups):
        hello((t + d) % groups, me)
    for s in range(2):
        g = group_of(2 * me + s)
        j = x * 2 + t // half

        @pl.when(jnp.logical_or(g != t, j != me))
        def _():
            hello(g, j)

    for g in range(groups):
        blk_s[g] = x_ref[g * piece : (g + 1) * piece]

    home = c == t // half
    own_copy = pltpu.make_async_copy(blk_s.at[clip], blk_r.at[t % half], loc.at[0])

    @pl.when(home)
    def _():
        own_copy.start()

    def times(axis, query):
        shape = (2 * rows, 1) if axis == 0 else (1, 2 * rows)
        at = lax.broadcasted_iota(jnp.int32, shape, axis)
        out = jnp.full(shape, FAR // 2 if query else FAR, jnp.int32)
        for f in range(groups):
            base = (f // half) * rows
            lo = base + lead + (f % half) * patch
            out = jnp.where((at >= lo) & (at < lo + patch), time_ref[f], out)
            lo = base + COND * (f % half)
            hi = lo + (COND if query else cond_ref[f])
            out = jnp.where((at >= lo) & (at < hi), time_ref[f], out)
        return out

    mask[...] = jnp.where(times(1, False) <= times(0, True), 0.0, -1e30)
    xs[0:lead] = jnp.zeros((lead, D), jnp.float32)

    targets = jnp.where(x == goal_x, half, 0)
    targets = targets - jnp.where((x == goal_x) & (goal == me) & home, 1, 0)
    pl.semaphore_wait(barrier, 3 + groups - 1 + targets)

    def enter(i):
        g = 2 * i + (t + x) % 2
        return g, remote(
            blk_s.at[clip_of(g)], blk_r.at[t % half], in_s.at[i], in_r.at[t % half], (g, me)
        )

    for i in range(half):
        g, copy = enter(i)

        @pl.when(home & (g != t))
        def _():
            copy.start()

    def span(j, first, count):
        return pl.ds(pl.multiple_of(j * width + first, share), count)

    def wo_own(l):
        at = wo.at[l, span(me, 0, width)]
        return remote(at, at, ws.at[l, OWN], wr.at[l, OWN], (t, partner))

    def wo_piece(l):
        at = wo.at[l, span(me, share * t, share)]
        return remote(at, at, ws.at[l, PIECE], wr.at[l, PIECE], (t, across))

    def wo_spread(l, d):
        at = wo.at[l, span(across, share * t, share)]
        return remote(
            at, at, ws.at[l, SPREAD + d], wr.at[l, SPREAD + d], ((t + d) % groups, me)
        )

    def wo_rest(l):
        at = wo.at[l, span(across, 0, width)]
        return remote(at, at, ws.at[l, REST], wr.at[l, REST], (t, partner))

    def wo_begin(l):
        weight_copy(l, 1).wait()
        wo_own(l).start()
        wo_piece(l).start()

    def wo_share(l):
        wo_piece(l).wait_recv()
        for d in range(1, groups):
            wo_spread(l, d).start()

    def wo_finish(l):
        for d in range(1, groups):
            wo_spread(l, d).wait_recv()
        wo_rest(l).start()

    def onward(k):
        return remote(blk_r.at[k], blk_r.at[k], fw_s.at[k], fw_r.at[k], (t, across))

    def arrival(k):
        return remote(blk_s.at[0], blk_r.at[k], in_s.at[0], in_r.at[k], (t, across))

    base = (x + t) % 2
    for i in range(half // 2):
        k = base + 2 * i
        mine = half * c + k == t

        @pl.when(jnp.logical_not(mine))
        def _():
            arrival(k).wait_recv()
            onward(k).start()

    wo_begin(0)
    wo_share(0)

    for i in range(half // 2):
        k = 1 - base + 2 * i
        mine = half * c + k == t

        @pl.when(jnp.logical_not(mine))
        def _():
            onward(k).wait_recv()

    @pl.when(home)
    def _():
        own_copy.wait()

    for k in range(half):
        block = blk_r[k].astype(jnp.float32)
        xs[lead + k * patch : lead + (k + 1) * patch] = block[:patch]
        xs[COND * k : COND * (k + 1)] = block[patch:]

    def norm(v, gain, bias):
        return layer_norm(v, gain, bias).astype(jnp.bfloat16)

    def in_half(h, r0, count):
        return pl.ds(pl.multiple_of(h * rows + r0, 16), count)

    def send1(l, i):
        r0, m = chunks[i]
        at = nrm1.at[l, c, pl.ds(r0, m)]
        return remote(at, at, ls.at[l, N1 + i], lr.at[l, N1 + i], (t, partner))

    def send2(l, i):
        r0, m = chunks[i]
        at = nrm2.at[l, c, pl.ds(r0, m)]
        return remote(at, at, ls.at[l, N2 + i], lr.at[l, N2 + i], (t, partner))

    def come1(l, i):
        r0, m = chunks[i]
        at = nrm1.at[l, 1 - c, pl.ds(r0, m)]
        return remote(at, at, ls.at[l, N1 + i], lr.at[l, N1 + i], (t, partner))

    def come2(l, i):
        r0, m = chunks[i]
        at = nrm2.at[l, 1 - c, pl.ds(r0, m)]
        return remote(at, at, ls.at[l, N2 + i], lr.at[l, N2 + i], (t, partner))

    def att_send(l, i, kind):
        r0, m = chunks[i]
        to = {AP: partner, AD: diagonal, AO: across}[kind]
        src = att.at[l, me, pl.ds(r0, m)] if kind == AO else att_p.at[l, pl.ds(r0, m)]
        return remote(
            src, att.at[l, me, pl.ds(r0, m)], ls.at[l, kind + i], lr.at[l, kind + i], (t, to)
        )

    def att_come(l, i, kind):
        r0, m = chunks[i]
        at = {AP: partner, AD: diagonal, AO: across}[kind]
        dst = att.at[l, at, pl.ds(r0, m)]
        return remote(dst, dst, ls.at[l, kind + i], lr.at[l, kind + i], (t, at))

    def sum_send(l, i):
        r0, m = chunks[i]
        at = pl.ds(r0, m)
        return remote(
            stg.at[l, at], rp.at[l, at], ls.at[l, RP + i], lr.at[l, RP + i], (t, partner)
        )

    def cross_send(l, i):
        r0, m = chunks[i]
        at = pl.ds(r0, m)
        return remote(us.at[l, at], ur.at[l, at], ls.at[l, XS + i], lr.at[l, XS + i], (t, across))

    def leave(k):
        return remote(
            out_s.at[k], out_r.at[clip % 2], os.at[k], orr.at[clip % 2], (half * c + k, goal)
        )

    def stay(k):
        return pltpu.make_async_copy(out_s.at[k], out_r.at[clip % 2], orr.at[clip % 2])

    for i, (r0, m) in enumerate(chunks):
        nrm1[0, c, r0 : r0 + m] = norm(xs[r0 : r0 + m], g1[0:1], b1[0:1])
        send1(0, i).start()

    lane = lax.broadcasted_iota(jnp.int32, (1, width), 1)
    heads = [(lane >= h * head_dim) & (lane < (h + 1) * head_dim) for h in range(head_local)]

    def layer(l, carry):
        weight_copy(l, 0).wait()

        def project(h, i):
            r0, m = chunks[i]
            normed = nrm1[l, h, r0 : r0 + m]
            for j, dst in enumerate((qb, kb, vb)):
                y = jnp.dot(normed, wqkv[l, j], preferred_element_type=jnp.float32)
                y = y + qkvb[j, pl.ds(l, 1)]
                if j == 0:
                    y = y * head_dim ** (-0.5)
                dst[in_half(h, r0, m)] = y.astype(jnp.bfloat16)

        for i in range(2):
            project(c, i)
        for i in range(2):
            come1(l, i).wait_recv()
            project(1 - c, i)

        def attend(h, i):
            r0, m = chunks[i]
            q = qb[in_half(h, r0, m)]
            stacked = jnp.concatenate(
                [q * jnp.where(on, 1.0, 0.0).astype(jnp.bfloat16) for on in heads], axis=0
            )
            sc = lax.dot_general(
                stacked, kb[...], (((1,), (1,)), ((), ())), preferred_element_type=jnp.float32
            )
            hide = mask[in_half(h, r0, m)]
            parts, totals = [], []
            for j in range(head_local):
                s = sc[j * m : (j + 1) * m] + hide
                w = jnp.exp(s - jnp.max(s, axis=-1, keepdims=True))
                totals.append(jnp.sum(w, axis=-1, keepdims=True))
                parts.append(w.astype(jnp.bfloat16))
            pv = jnp.dot(
                jnp.concatenate(parts, axis=0), vb[...], preferred_element_type=jnp.float32
            )
            acc = jnp.zeros((m, width), jnp.float32)
            for j in range(head_local):
                acc = jnp.where(heads[j], pv[j * m : (j + 1) * m] * (1.0 / totals[j]), acc)
            return acc.astype(jnp.bfloat16)

        for i, (r0, m) in enumerate(chunks):
            att_p[l, r0 : r0 + m] = attend(1 - c, i)
            att_send(l, i, AD).start()
            att_send(l, i, AP).start()
            att[l, me, r0 : r0 + m] = attend(c, i)
            att_send(l, i, AO).start()
            if i == 0:
                wo_finish(l)

        @pl.when(l < last)
        def _():
            wo_begin(l + 1)
            wo_share(l + 1)

        wo_own(l).wait_recv()
        wo_rest(l).wait_recv()
        for i, (r0, m) in enumerate(chunks):
            for kind in (AP, AD, AO):
                att_come(l, i, kind).wait_recv()
            full = jnp.concatenate([att[l, j, r0 : r0 + m] for j in range(4)], axis=1)
            first = jnp.dot(full, wo[l], preferred_element_type=jnp.float32)
            first = xs[r0 : r0 + m] + first + ob[pl.ds(l, 1)]
            xs[r0 : r0 + m] = first
            nrm2[l, c, r0 : r0 + m] = norm(first, g2[pl.ds(l, 1)], b2[pl.ds(l, 1)])
            send2(l, i).start()

        weight_copy(l, 2).wait()
        weight_copy(l, 3).wait()

        def mlp(h, i):
            r0, m = chunks[i]
            normed = nrm2[l, h, r0 : r0 + m]
            tile = 256
            for n in range(w1.shape[2] // tile):
                at = pl.ds(n * tile, tile)
                y = jnp.dot(normed, w1[l, :, at], preferred_element_type=jnp.float32)
                y = y + f1b[pl.ds(l, 1), at]
                y = 0.5 * y * (1.0 + lax.erf(y * (0.5**0.5)))
                inner[0:m, at] = y.astype(jnp.bfloat16)
            return jnp.dot(inner[0:m], w2[l], preferred_element_type=jnp.float32)

        sends_x = jnp.logical_or(l < last, x != goal_x)
        takes_x = jnp.logical_or(l < last, x == goal_x)

        def combine(i):
            r0, m = chunks[i]
            sum_send(l, i).wait_recv()
            u = keep[r0 : r0 + m] + rp[l, r0 : r0 + m].astype(jnp.float32)
            keep[r0 : r0 + m] = u
            us[l, r0 : r0 + m] = u.astype(jnp.bfloat16)

            @pl.when(sends_x)
            def _():
                cross_send(l, i).start()

        for i, (r0, m) in enumerate(chunks):
            keep[r0 : r0 + m] = mlp(c, i)
            if i > 0:
                combine(i - 1)
            come2(l, i).wait_recv()
            stg[l, r0 : r0 + m] = mlp(1 - c, i).astype(jnp.bfloat16)
            sum_send(l, i).start()
        combine(1)

        for i, (r0, m) in enumerate(chunks):

            @pl.when(takes_x)
            def _():
                cross_send(l, i).wait_recv()
                new = xs[r0 : r0 + m] + keep[r0 : r0 + m] + f2b[pl.ds(l, 1)]
                new = (new + ur[l, r0 : r0 + m].astype(jnp.float32)).astype(jnp.bfloat16)

                @pl.when(l < last)
                def _():
                    wide = new.astype(jnp.float32)
                    xs[r0 : r0 + m] = wide
                    nrm1[l + 1, c, r0 : r0 + m] = norm(
                        wide, g1[pl.ds(l + 1, 1)], b1[pl.ds(l + 1, 1)]
                    )
                    send1(l + 1, i).start()

                @pl.when(l == last)
                def _():
                    if i == 0:
                        for k in range(half):
                            out_s[k, patch:piece] = new[COND * k : COND * (k + 1)]
                    skip = lead if i == 0 else 0
                    for k in range(half // 2):
                        block = new[skip + k * patch : skip + (k + 1) * patch]
                        out_s[k + i * (half // 2), 0:patch] = block
                    for k in range(i * (half // 2), (i + 1) * (half // 2)):
                        here = (half * c + k == t) & (goal == me)

                        @pl.when(here)
                        def _():
                            stay(k).start()

                        @pl.when(jnp.logical_not(here))
                        def _():
                            leave(k).start()

        for i in range(2):
            send1(l, i).wait_send()
            send2(l, i).wait_send()
            for kind in (AP, AD, AO):
                att_send(l, i, kind).wait_send()
            sum_send(l, i).wait_send()

            @pl.when(sends_x)
            def _():
                cross_send(l, i).wait_send()

        wo_own(l).wait_send()
        wo_piece(l).wait_send()
        wo_rest(l).wait_send()
        for d in range(1, groups):
            wo_spread(l, d).wait_send()
        return carry

    lax.fori_loop(0, LAYERS, layer, 0)

    for i in range(half):
        g, copy = enter(i)

        @pl.when(home & (g != t))
        def _():
            copy.wait_send()

    for i in range(half // 2):
        k = base + 2 * i

        @pl.when(half * c + k != t)
        def _():
            onward(k).wait_send()

    for s in range(2):
        there = 2 * me + s
        here = (group_of(there) == t) & (x * 2 + t // half == me)

        @pl.when(here)
        def _():
            pltpu.make_async_copy(out_s.at[t % half], out_r.at[s], orr.at[s]).wait()

        @pl.when(jnp.logical_not(here))
        def _():
            remote(out_s.at[0], out_r.at[s], os.at[0], orr.at[s], (t, across)).wait_recv()

        out_ref[s * piece : (s + 1) * piece] = out_r[s]

    for k in range(half):
        here = (half * c + k == t) & (goal == me)

        @pl.when((x == goal_x) & jnp.logical_not(here))
        def _():
            leave(k).wait_send()


def shards_clip(
    frames_in,
    frame_time,
    cond_count,
    ln1_gain,
    ln1_bias,
    qkv_weight,
    qkv_bias,
    out_weight,
    out_bias,
    ln2_gain,
    ln2_bias,
    fc1_weight,
    fc1_bias,
    fc2_weight,
    fc2_bias,
):
    groups = lax.axis_size("tm")
    tensor_size = lax.axis_size("tensor")
    piece = PATCH_DEV + COND
    half = groups // 2
    width = qkv_weight.shape[3]
    hidden = fc1_weight.shape[2]
    lead = -(-half * COND // 16) * 16
    rows = lead + half * PATCH_DEV
    cut = lead + (half // 2) * PATCH_DEV

    vmem = pl.BlockSpec(memory_space=pltpu.VMEM)
    smem = pl.BlockSpec(memory_space=pltpu.SMEM)
    hbm = pl.BlockSpec(memory_space=pl.ANY)
    bf16, f32 = jnp.bfloat16, jnp.float32
    dma = pltpu.SemaphoreType.DMA
    out = pl.pallas_call(
        clip_kernel,
        out_shape=jax.ShapeDtypeStruct((2 * piece, D), bf16),
        in_specs=[vmem, smem, smem] + [vmem] * 8 + [hbm] * 4,
        out_specs=vmem,
        scratch_shapes=[
            pltpu.VMEM(qkv_weight.shape, bf16),
            pltpu.VMEM((LAYERS, D, D), bf16),
            pltpu.VMEM(fc1_weight.shape, bf16),
            pltpu.VMEM(fc2_weight.shape, bf16),
            pltpu.VMEM((groups, piece, D), bf16),
            pltpu.VMEM((half, piece, D), bf16),
            pltpu.VMEM((rows, D), f32),
            pltpu.VMEM((rows, D), f32),
            pltpu.VMEM((LAYERS, 2, rows, D), bf16),
            pltpu.VMEM((LAYERS, 2, rows, D), bf16),
            pltpu.VMEM((2 * rows, width), bf16),
            pltpu.VMEM((2 * rows, width), bf16),
            pltpu.VMEM((2 * rows, width), bf16),
            pltpu.VMEM((2 * rows, 2 * rows), f32),
            pltpu.VMEM((LAYERS, tensor_size, rows, width), bf16),
            pltpu.VMEM((LAYERS, rows, width), bf16),
            pltpu.VMEM((cut, hidden), bf16),
            pltpu.VMEM((LAYERS, rows, D), bf16),
            pltpu.VMEM((LAYERS, rows, D), bf16),
            pltpu.VMEM((LAYERS, rows, D), bf16),
            pltpu.VMEM((LAYERS, rows, D), bf16),
            pltpu.VMEM((half, piece, D), bf16),
            pltpu.VMEM((2, piece, D), bf16),
            dma((LAYERS, 4)),
            dma((half,)),
            dma((half,)),
            dma((half,)),
            dma((half,)),
            dma((1,)),
            dma((LAYERS, IDS)),
            dma((LAYERS, IDS)),
            dma((LAYERS, SPREAD + groups)),
            dma((LAYERS, SPREAD + groups)),
            dma((half,)),
            dma((2,)),
        ],
        compiler_params=pltpu.CompilerParams(
            collective_id=0, has_side_effects=True, vmem_limit_bytes=60 * 1024 * 1024
        ),
    )(
        frames_in[0],
        frame_time,
        cond_count,
        ln1_gain,
        ln1_bias,
        qkv_bias.transpose(1, 0, 2),
        out_bias,
        ln2_gain,
        ln2_bias,
        fc1_bias,
        fc2_bias,
        qkv_weight,
        out_weight,
        fc1_weight,
        fc2_weight,
    )
    return out[None]


def shards(frames_in, frame_time, cond_count, *rest):
    groups = lax.axis_size("tm")
    seq_count = frames_in.shape[1] // (PATCH_DEV + COND)
    by_clip = frame_time.shape[0] == groups and seq_count == groups
    by_clip = by_clip and lax.axis_size("tensor") == 4 and groups == 8
    body = shards_clip if by_clip else shards_gather
    return body(frames_in, frame_time, cond_count, *rest)


def solution(mesh):
    in_specs = (
        P("tm", None, None),
        P(),
        P(),
        P(),
        P(),
        P(None, None, None, "tensor"),
        P(None, None, "tensor"),
        P(None, "tensor", None),
        P(),
        P(),
        P(),
        P(None, None, "tensor"),
        P(None, "tensor"),
        P(None, "tensor", None),
        P(),
    )
    out_specs = P("tm", "tensor", None)
    return jax.shard_map(shards, mesh=mesh, in_specs=in_specs, out_specs=out_specs, check_vma=False)
```

```python
import jax
import jax.numpy as jnp
from jax import lax
from jax.experimental import pallas as pl
from jax.experimental.pallas import tpu as pltpu
from jax.sharding import PartitionSpec as P

D = 1024
HEADS = 16
PATCH_DEV = 64
COND = 2
LAYERS = 2


def layer_norm(inputs, gain_row, bias_row):
    center = jnp.mean(inputs, axis=-1, keepdims=True)
    spread = jnp.mean(jnp.square(inputs - center), axis=-1, keepdims=True)
    return (inputs - center) * lax.rsqrt(spread + 1e-06) * gain_row + bias_row


def piece_tables(frame_time, cond_count, piece_count, frame_split, piece_rows):
    cond_dev = COND // frame_split
    piece_ids = jnp.arange(piece_count, dtype=jnp.int32)
    frame_ids = jnp.arange(frame_time.shape[0], dtype=jnp.int32)
    matches = (piece_ids // frame_split)[:, None] == frame_ids[None, :]
    piece_time = jnp.sum(jnp.where(matches, frame_time[None, :], 0), axis=1)
    piece_cond = jnp.sum(jnp.where(matches, cond_count[None, :], 0), axis=1)
    slot_index = jnp.arange(piece_rows, dtype=jnp.int32)
    cond_slot = (piece_ids % frame_split)[:, None] * cond_dev + slot_index[None, :] - PATCH_DEV
    valid = (slot_index[None, :] < PATCH_DEV) | (cond_slot < piece_cond[:, None])
    return (piece_time, valid)


def shards_gather(
    frames_in,
    frame_time,
    cond_count,
    ln1_gain,
    ln1_bias,
    qkv_weight,
    qkv_bias,
    out_weight,
    out_bias,
    ln2_gain,
    ln2_bias,
    fc1_weight,
    fc1_bias,
    fc2_weight,
    fc2_bias,
):
    frame_count = frame_time.shape[0]
    piece_count = lax.axis_size("tm")
    frame_split = piece_count // frame_count
    cond_dev = COND // frame_split
    piece_rows = PATCH_DEV + cond_dev
    row_count = frames_in.shape[1]
    seq_count = row_count // piece_rows
    head_dim = D // HEADS
    head_local = qkv_weight.shape[3] // head_dim
    scale = head_dim ** (-0.5)
    tensor_size = lax.axis_size("tensor")
    tensor_pos = lax.axis_index("tensor")
    my_piece = lax.axis_index("tm")
    share_rows = row_count // tensor_size
    piece_time, valid = piece_tables(frame_time, cond_count, piece_count, frame_split, piece_rows)
    piece_ids = jnp.arange(piece_count, dtype=jnp.int32)
    my_time = jnp.sum(jnp.where(piece_ids == my_piece, piece_time, 0))
    full_in = frames_in[0]
    new_share = None
    for layer_idx in range(LAYERS):
        normed = layer_norm(
            full_in.astype(jnp.float32), ln1_gain[layer_idx], ln1_bias[layer_idx]
        ).astype(jnp.bfloat16)
        projected = jnp.einsum(
            "rd,jde->jre", normed, qkv_weight[layer_idx], preferred_element_type=jnp.float32
        )
        projected = (projected + qkv_bias[layer_idx][:, None, :]).astype(jnp.bfloat16)
        queries = projected[0].reshape(seq_count, piece_rows, head_local, head_dim)
        keys_mine = projected[1].reshape(1, seq_count, piece_rows, head_local * head_dim)
        values_mine = projected[2].reshape(1, seq_count, piece_rows, head_local * head_dim)
        start_top = jnp.full((seq_count, head_local, piece_rows), -1e30, jnp.float32)
        key_block = lax.all_gather(keys_mine, "tm", axis=0, tiled=True)
        value_block = lax.all_gather(values_mine, "tm", axis=0, tiled=True)
        block_count = key_block.shape[0]
        block_ids = jnp.arange(block_count, dtype=jnp.int32)
        matches = block_ids[:, None] == piece_ids[None, :]
        key_time = jnp.sum(jnp.where(matches, piece_time[None, :], 0), axis=1)
        key_valid = jnp.any(matches[:, :, None] & valid[None, :, :], axis=1)
        allowed = (key_time <= my_time)[:, None] & key_valid
        top_run = start_top
        keys_split = key_block.reshape(block_count, seq_count, piece_rows, head_local, head_dim)
        values_split = value_block.reshape(block_count, seq_count, piece_rows, head_local, head_dim)
        scores = (
            jnp.einsum("sqhd,gskhd->shqgk", queries, keys_split, preferred_element_type=jnp.float32)
            * scale
        )
        scores = jnp.where(allowed, scores, -1e30)
        new_top = jnp.maximum(top_run, jnp.max(scores, axis=(3, 4)))
        weights = jnp.where(allowed, jnp.exp(scores - new_top[..., None, None]), 0.0)
        total_new = jnp.sum(weights, axis=(3, 4))
        mixed = jnp.einsum(
            "shqgk,gskhd->shqd",
            weights.astype(jnp.bfloat16),
            values_split,
            preferred_element_type=jnp.float32,
        )
        top_run = new_top
        attended = (
            (mixed / total_new[..., None])
            .transpose(0, 2, 1, 3)
            .reshape(row_count, head_local * head_dim)
            .astype(jnp.bfloat16)
        )
        out_layer = out_weight[layer_idx]
        fc1_layer = fc1_weight[layer_idx]
        fc2_layer = fc2_weight[layer_idx]
        fc1_layer_bias = fc1_bias[layer_idx]
        own_rows = lax.dynamic_slice_in_dim(full_in, tensor_pos * share_rows, share_rows, 0).astype(
            jnp.float32
        )
        first = (
            own_rows
            + lax.psum_scatter(
                jnp.dot(attended, out_layer, preferred_element_type=jnp.float32).astype(
                    jnp.bfloat16
                ),
                "tensor",
                scatter_dimension=0,
                tiled=True,
            ).astype(jnp.float32)
            + out_bias[layer_idx]
        )
        normed_two = layer_norm(first, ln2_gain[layer_idx], ln2_bias[layer_idx]).astype(
            jnp.bfloat16
        )
        inner = jax.nn.gelu(
            jnp.dot(
                lax.all_gather(normed_two, "tensor", axis=0, tiled=True),
                fc1_layer,
                preferred_element_type=jnp.float32,
            )
            + fc1_layer_bias,
            approximate=False,
        ).astype(jnp.bfloat16)
        mlp_share = lax.psum_scatter(
            jnp.dot(inner, fc2_layer, preferred_element_type=jnp.float32).astype(jnp.bfloat16),
            "tensor",
            scatter_dimension=0,
            tiled=True,
        ).astype(jnp.float32)
        new_share = (first + mlp_share + fc2_bias[layer_idx]).astype(jnp.bfloat16)
        if layer_idx + 1 < LAYERS:
            full_in = lax.all_gather(new_share, "tensor", axis=0, tiled=True)
    return new_share[None]


MESH = pl.DeviceIdType.MESH
FAR = 1 << 30
N1, AP, AD, AO, XS = range(5)
OWN, PIECE, REST, UP, DOWN, SPREAD = range(6)


def clip_kernel(
    x_ref, time_ref, cond_ref, g1, b1, qkvb, ob, g2, b2, f1b, f2b, wqkv_h, wo_h, w1_h, w2_h,
    out_ref, wqkv, wo, w1, w2, w1p, w2p, f1p, blk_s, blk_r, xs, keep, nrm1, nrm2, qb, kb, vb, mask,
    att, att_p, inner, us, ur, out_s, out_r,
    wsem, in_s, in_r, fw_s, fw_r, loc, bs, br, ls, lr, ws, wr, os, orr,
):
    groups = blk_s.shape[0]
    half = blk_r.shape[0]
    piece = blk_r.shape[1]
    patch = PATCH_DEV
    rows = xs.shape[0]
    lead = rows - half * patch
    chunks = [(lead + i * patch, patch) for i in range(half)]
    chunks[0] = (0, lead + patch)
    cut = lead + (half // 2) * patch
    spans = ((0, cut), (cut, rows - cut))
    per = half // 2
    head_dim = D // HEADS
    width = qb.shape[1]
    head_local = width // head_dim
    share = width // groups
    last = LAYERS - 1

    t = lax.axis_index("tm")
    me = lax.axis_index("tensor")
    x = me // 2
    c = me % 2
    partner = me + 1 - 2 * c
    beside = t + 1 - 2 * (t % 2)
    across = (me + 2) % 4
    diagonal = (partner + 2) % 4

    def clip_of(g):
        return g // 2 + half * ((g // 2 + g) % 2)

    def group_of(clip):
        z = clip % half
        return 2 * z + (clip // half + z) % 2

    clip = clip_of(t)
    goal_x = clip // half
    goal = clip // 2

    pairs = ((wqkv_h, wqkv), (wo_h, wo), (w1_h, w1), (w2_h, w2))

    def weight_copy(l, j):
        dst = pairs[j][1].at[l]
        if j == 1:
            dst = wo.at[l, pl.ds(pl.multiple_of(me * width, width), width)]
        return pltpu.make_async_copy(pairs[j][0].at[l], dst, wsem.at[l, j])

    for l in range(LAYERS):
        for j in ((1, 0, 2, 3) if l == 0 else (0, 1, 2, 3)):
            weight_copy(l, j).start()

    def remote(src, dst, s, r, to):
        return pltpu.make_async_remote_copy(
            src_ref=src, dst_ref=dst, send_sem=s, recv_sem=r, device_id=to, device_id_type=MESH
        )

    barrier = pltpu.get_barrier_semaphore()

    def hello(g, j):
        pl.semaphore_signal(barrier, inc=1, device_id=(g, j), device_id_type=MESH)

    for other in (partner, across, diagonal):
        hello(t, other)
    for d in range(1, groups):
        hello((t + d) % groups, me)
    for s in range(2):
        g = group_of(2 * me + s)
        j = x * 2 + t // half

        @pl.when(jnp.logical_or(g != t, j != me))
        def _():
            hello(g, j)

    for g in range(groups):
        blk_s[g] = x_ref[g * piece : (g + 1) * piece]

    home = c == t // half
    own_copy = pltpu.make_async_copy(blk_s.at[clip], blk_r.at[t % half], loc.at[0])

    @pl.when(home)
    def _():
        own_copy.start()

    def times(axis, query):
        shape = (2 * rows, 1) if axis == 0 else (1, 2 * rows)
        at = lax.broadcasted_iota(jnp.int32, shape, axis)
        out = jnp.full(shape, FAR // 2 if query else FAR, jnp.int32)
        for f in range(groups):
            base = (f // half) * rows
            lo = base + lead + (f % half) * patch
            out = jnp.where((at >= lo) & (at < lo + patch), time_ref[f], out)
            lo = base + COND * (f % half)
            hi = lo + (COND if query else cond_ref[f])
            out = jnp.where((at >= lo) & (at < hi), time_ref[f], out)
        return out

    mask[...] = jnp.where(times(1, False) <= times(0, True), 0.0, -1e30)
    xs[0:lead] = jnp.zeros((lead, D), jnp.float32)

    targets = jnp.where(x == goal_x, half, 0)
    targets = targets - jnp.where((x == goal_x) & (goal == me) & home, 1, 0)
    with jax.named_scope("barrier"):
        pl.semaphore_wait(barrier, 3 + groups - 1 + targets)

    def enter(i):
        far = jnp.where(x == 0, t // 2 + 2, half - 1 - t // 2)
        z = (far + 2 * (i // 2)) % half
        g = 2 * z + i % 2
        return g, remote(
            blk_s.at[clip_of(g)], blk_r.at[t % half], in_s.at[i], in_r.at[t % half], (g, me)
        )

    for i in range(half):
        g, copy = enter(i)

        @pl.when(home & (g != t))
        def _():
            copy.start()

    def span(j, first, count):
        return pl.ds(pl.multiple_of(j * width + first, share), count)

    def wo_own(l):
        at = wo.at[l, span(me, 0, width)]
        return remote(at, at, ws.at[l, OWN], wr.at[l, OWN], (t, partner))

    def wo_piece(l):
        at = wo.at[l, span(me, share * t, share)]
        return remote(at, at, ws.at[l, PIECE], wr.at[l, PIECE], (t, across))

    def wo_slice(l, g):
        return wo.at[l, span(across, share * g, share)]

    def wo_column(l, d, g):
        at = wo_slice(l, g)
        to = (t + 2 * d) % groups
        return remote(at, at, ws.at[l, SPREAD + d], wr.at[l, SPREAD + d], (to, me))

    def wo_row(l, d, g):
        at = wo_slice(l, g)
        j = SPREAD + half + d
        return remote(at, at, ws.at[l, j], wr.at[l, j], (beside, me))

    def wo_rest(l):
        at = wo.at[l, span(across, 0, width)]
        return remote(at, at, ws.at[l, REST], wr.at[l, REST], (t, partner))

    def mlp_weights(l):
        return [
            remote(src.at[l], dst.at[l], ws.at[l, j], wr.at[l, j], (t, partner))
            for j, src, dst in ((UP, w1_h, w1p), (DOWN, w2_h, w2p))
        ]

    def wo_begin(l):
        weight_copy(l, 1).wait()
        wo_piece(l).start()
        wo_own(l).start()

    def wo_share(l):
        wo_piece(l).wait_recv()
        for d in range(1, half):
            wo_column(l, d, t).start()
        wo_row(l, 0, t).start()

    def wo_relay(l):
        for d in range(1, half):
            g = (t - 2 * d + groups) % groups
            wo_column(l, d, g).wait_recv()
            wo_row(l, d, g).start()

    def wo_finish(l):
        for d in range(half):
            wo_row(l, d, (beside - 2 * d + groups) % groups).wait_recv()
        wo_rest(l).start()

    bias_copy = remote(f1b, f1p, bs.at[0], br.at[0], (t, partner))
    wo_begin(0)
    bias_copy.start()
    for copy in mlp_weights(0):
        copy.start()

    def onward(k):
        return remote(blk_r.at[k], blk_r.at[k], fw_s.at[k], fw_r.at[k], (t, across))

    def arrival(k):
        return remote(blk_s.at[0], blk_r.at[k], in_s.at[0], in_r.at[k], (t, across))

    first_k = per * ((t // 2 + x) % 2)
    with jax.named_scope("wo_first"):
        wo_share(0)

    for i in range(per):
        k = first_k + i

        @pl.when(half * c + k != t)
        def _():
            with jax.named_scope("in_direct"):
                arrival(k).wait_recv()
            onward(k).start()

    def norm(v, gain, bias):
        return layer_norm(v, gain, bias).astype(jnp.bfloat16)

    def in_half(h, r0, count):
        return pl.ds(pl.multiple_of(h * rows + r0, 16), count)

    def ids(l, kind, i):
        return ls.at[l, kind * (half + 1) + i], lr.at[l, kind * (half + 1) + i]

    def normed_send(l, i):
        at = nrm1.at[l, c, pl.ds(*chunks[i])]
        return remote(at, at, *ids(l, N1, i), (t, partner))

    def normed_come(l, i):
        at = nrm1.at[l, 1 - c, pl.ds(*chunks[i])]
        return remote(at, at, *ids(l, N1, i), (t, partner))

    def att_send(l, i, kind):
        at = pl.ds(*spans[i])
        to = {AP: partner, AD: diagonal, AO: across}[kind]
        src = att.at[l, me, at] if kind == AO else att_p.at[l, at]
        return remote(src, att.at[l, me, at], *ids(l, kind, i), (t, to))

    def att_come(l, i, kind):
        to = {AP: partner, AD: diagonal, AO: across}[kind]
        dst = att.at[l, to, pl.ds(*spans[i])]
        return remote(dst, dst, *ids(l, kind, i), (t, to))

    def cross_send(l, i):
        at = pl.ds(*chunks[i])
        return remote(us.at[l, at], ur.at[l, at], *ids(l, XS, i), (t, across))

    def leave(k):
        return remote(
            out_s.at[k], out_r.at[clip % 2], os.at[k], orr.at[clip % 2], (half * c + k, goal)
        )

    def stay(k):
        return pltpu.make_async_copy(out_s.at[k], out_r.at[clip % 2], orr.at[clip % 2])

    def project(l, h, r0, m):
        at = pl.ds(r0 if isinstance(r0, int) else pl.multiple_of(r0, 16), m)
        normed = nrm1[l, h, at]
        for j, dst in enumerate((qb, kb, vb)):
            y = jnp.dot(normed, wqkv[l, j], preferred_element_type=jnp.float32)
            y = y + qkvb[j, pl.ds(l, 1)]
            if j == 0:
                y = y * head_dim ** (-0.5)
            dst[in_half(h, r0, m)] = y.astype(jnp.bfloat16)

    def strip(i):
        return pl.ds(pl.multiple_of(lead + i * patch, 16), patch) if i is not None else pl.ds(0, lead)

    def block_send(h, i):
        at = nrm1.at[0, h, strip(i)]
        return remote(at, at, *ids(0, N1, half if i is None else i), (t, partner))

    def normed_in(i):
        at = strip(i)
        nrm1[0, c, at] = norm(xs[at], g1[0:1], b1[0:1])
        block_send(c, i).start()

    def take(k):
        xs[strip(k)] = blk_r[k, 0:patch].astype(jnp.float32)
        normed_in(k)
        project(0, c, lead + k * patch, patch)

    def take_other(k):
        with jax.named_scope("n1_wait"):
            block_send(1 - c, k).wait_recv()
        project(0, 1 - c, lead + k * patch, patch)

    weight_copy(0, 0).wait()
    for i in range(per):
        k = first_k + i

        @pl.when(half * c + k == t)
        def _():
            own_copy.wait()

        take(k)
    with jax.named_scope("wo_relay"):
        wo_relay(0)
    for i in range(per):
        k = per - first_k + i

        @pl.when(half * c + k == t)
        def _():
            own_copy.wait()

        @pl.when(half * c + k != t)
        def _():
            with jax.named_scope("in_cross"):
                onward(k).wait_recv()

        take(k)
        take_other(first_k + i)
    for k in range(half):
        xs[COND * k : COND * (k + 1)] = blk_r[k, patch:piece].astype(jnp.float32)
    normed_in(None)
    for l in range(1, LAYERS):
        wo_begin(l)
    project(0, c, 0, lead)
    for i in range(per):
        take_other(per - first_k + i)
    block_send(1 - c, None).wait_recv()
    project(0, 1 - c, 0, lead)

    lane = lax.broadcasted_iota(jnp.int32, (1, width), 1)
    heads = [(lane >= h * head_dim) & (lane < (h + 1) * head_dim) for h in range(head_local)]

    def layer(l, carry):
        def attend(h, r0, m):
            q = qb[in_half(h, r0, m)]
            stacked = jnp.concatenate(
                [q * jnp.where(on, 1.0, 0.0).astype(jnp.bfloat16) for on in heads], axis=0
            )
            sc = lax.dot_general(
                stacked, kb[...], (((1,), (1,)), ((), ())), preferred_element_type=jnp.float32
            )
            hide = mask[in_half(h, r0, m)]
            parts, totals = [], []
            for j in range(head_local):
                s = sc[j * m : (j + 1) * m] + hide
                w = jnp.exp(s - jnp.max(s, axis=-1, keepdims=True))
                totals.append(jnp.sum(w, axis=-1, keepdims=True))
                parts.append(w.astype(jnp.bfloat16))
            pv = jnp.dot(
                jnp.concatenate(parts, axis=0), vb[...], preferred_element_type=jnp.float32
            )
            acc = jnp.zeros((m, width), jnp.float32)
            for j in range(head_local):
                acc = jnp.where(heads[j], pv[j * m : (j + 1) * m] * (1.0 / totals[j]), acc)
            return acc.astype(jnp.bfloat16)

        for i, (r0, m) in enumerate(spans):
            with jax.named_scope("attend_other"):
                att_p[l, r0 : r0 + m] = attend(1 - c, r0, m)
            att_send(l, i, AD).start()
            att_send(l, i, AP).start()
            with jax.named_scope("attend_own"):
                att[l, me, r0 : r0 + m] = attend(c, r0, m)
            att_send(l, i, AO).start()
            if i == 0:
                with jax.named_scope("wo_finish"):
                    wo_finish(l)

        @pl.when(l < last)
        def _():
            for copy in mlp_weights(l + 1):
                copy.start()

        with jax.named_scope("wo_rest_wait"):
            wo_own(l).wait_recv()
            wo_rest(l).wait_recv()
        weight_copy(l, 2).wait()
        weight_copy(l, 3).wait()

        def ready(i, r0, m):
            with jax.named_scope("att_wait"):
                for kind in (AP, AD, AO):
                    att_come(l, i, kind).wait_recv()
            full = jnp.concatenate([att[l, j, r0 : r0 + m] for j in range(4)], axis=1)
            first = jnp.dot(full, wo[l], preferred_element_type=jnp.float32)
            first = xs[r0 : r0 + m] + first + ob[pl.ds(l, 1)]
            xs[r0 : r0 + m] = first
            nrm2[0:m] = norm(first, g2[pl.ds(l, 1)], b2[pl.ds(l, 1)])

        def mlp(m):
            tile = 256
            hidden = w1.shape[2]
            total = 0.0
            for p, (up, bias, down) in enumerate(((w1, f1b, w2), (w1p, f1p, w2p))):
                for n in range(hidden // tile):
                    at = pl.ds(n * tile, tile)
                    y = jnp.dot(nrm2[0:m], up[l, :, at], preferred_element_type=jnp.float32)
                    y = y + bias[pl.ds(l, 1), at]
                    y = 0.5 * y * (1.0 + lax.erf(y * (0.5**0.5)))
                    inner[0:m, pl.ds(n * tile, tile)] = y.astype(jnp.bfloat16)
                total = total + jnp.dot(
                    inner[0:m], down[l], preferred_element_type=jnp.float32
                )
            return total

        sends_x = jnp.logical_or(l < last, x != goal_x)
        takes_x = jnp.logical_or(l < last, x == goal_x)

        for i, (r0, m) in enumerate(spans):
            ready(i, r0, m)
            if i == 0:
                with jax.named_scope("weights_wait"):

                    @pl.when(l == 0)
                    def _():
                        bias_copy.wait_recv()

                    for copy in mlp_weights(l):
                        copy.wait_recv()
            with jax.named_scope("mlp"):
                u = mlp(m)
                keep[r0 : r0 + m] = u
                us[l, r0 : r0 + m] = u.astype(jnp.bfloat16)

            @pl.when(sends_x)
            def _():
                for j in range(per * i, per * (i + 1)):
                    cross_send(l, j).start()

            if i == 0:

                @pl.when(l < last)
                def _():
                    wo_share(l + 1)

        @pl.when(l < last)
        def _():
            weight_copy(l + 1, 0).wait()

        def other(i):
            with jax.named_scope("n1_wait"):
                normed_come(l + 1, i).wait_recv()
            project(l + 1, 1 - c, *chunks[i])

        for i, (r0, m) in enumerate(chunks):

            @pl.when(takes_x)
            def _():
                with jax.named_scope("x_wait"):
                    cross_send(l, i).wait_recv()
                new = xs[r0 : r0 + m] + keep[r0 : r0 + m] + f2b[pl.ds(l, 1)]
                new = (new + ur[l, r0 : r0 + m].astype(jnp.float32)).astype(jnp.bfloat16)

                @pl.when(l < last)
                def _():
                    wide = new.astype(jnp.float32)
                    xs[r0 : r0 + m] = wide
                    nrm1[l + 1, c, r0 : r0 + m] = norm(
                        wide, g1[pl.ds(l + 1, 1)], b1[pl.ds(l + 1, 1)]
                    )
                    normed_send(l + 1, i).start()
                    project(l + 1, c, r0, m)
                    if i > 0:
                        other(i - 1)

                @pl.when(l == last)
                def _():
                    if i == 0:
                        for k in range(half):
                            out_s[k, patch:piece] = new[COND * k : COND * (k + 1)]
                    out_s[i, 0:patch] = new[m - patch :]
                    here = (half * c + i == t) & (goal == me)

                    @pl.when(here)
                    def _():
                        stay(i).start()

                    @pl.when(jnp.logical_not(here))
                    def _():
                        leave(i).start()

            if i == half - 3:

                @pl.when(l < last)
                def _():
                    with jax.named_scope("wo_relay"):
                        wo_relay(l + 1)

        @pl.when(l < last)
        def _():
            other(half - 1)

        return carry

    lax.fori_loop(0, LAYERS, layer, 0)

    for i in range(half):
        g, copy = enter(i)

        @pl.when(home & (g != t))
        def _():
            copy.wait_send()

    for i in range(per):
        k = first_k + i

        @pl.when(half * c + k != t)
        def _():
            onward(k).wait_send()

    for s in range(2):
        there = 2 * me + s
        here = (group_of(there) == t) & (x * 2 + t // half == me)

        @pl.when(here)
        def _():
            pltpu.make_async_copy(out_s.at[t % half], out_r.at[s], orr.at[s]).wait()

        @pl.when(jnp.logical_not(here))
        def _():
            with jax.named_scope("out_wait"):
                remote(out_s.at[0], out_r.at[s], os.at[0], orr.at[s], (t, across)).wait_recv()

        out_ref[s * piece : (s + 1) * piece] = out_r[s]

    for k in range(half):
        here = (half * c + k == t) & (goal == me)

        @pl.when((x == goal_x) & jnp.logical_not(here))
        def _():
            leave(k).wait_send()

    bias_copy.wait_send()

    for i in range(half):
        block_send(c, i).wait_send()
    block_send(c, None).wait_send()

    def drain(l, carry):
        for i in range(half):

            @pl.when(l > 0)
            def _():
                normed_send(l, i).wait_send()

            @pl.when(jnp.logical_or(l < last, x != goal_x))
            def _():
                cross_send(l, i).wait_send()

        for i in range(len(spans)):
            for kind in (AP, AD, AO):
                att_send(l, i, kind).wait_send()

        wo_own(l).wait_send()
        wo_piece(l).wait_send()
        wo_rest(l).wait_send()
        for d in range(1, half):
            wo_column(l, d, t).wait_send()
        for d in range(half):
            wo_row(l, d, t).wait_send()
        for copy in mlp_weights(l):
            copy.wait_send()
        return carry

    lax.fori_loop(0, LAYERS, drain, 0)


def shards_clip(
    frames_in,
    frame_time,
    cond_count,
    ln1_gain,
    ln1_bias,
    qkv_weight,
    qkv_bias,
    out_weight,
    out_bias,
    ln2_gain,
    ln2_bias,
    fc1_weight,
    fc1_bias,
    fc2_weight,
    fc2_bias,
):
    groups = lax.axis_size("tm")
    tensor_size = lax.axis_size("tensor")
    piece = PATCH_DEV + COND
    half = groups // 2
    width = qkv_weight.shape[3]
    hidden = fc1_weight.shape[2]
    lead = -(-half * COND // 16) * 16
    rows = lead + half * PATCH_DEV
    chunk = lead + (half // 2) * PATCH_DEV

    vmem = pl.BlockSpec(memory_space=pltpu.VMEM)
    smem = pl.BlockSpec(memory_space=pltpu.SMEM)
    hbm = pl.BlockSpec(memory_space=pl.ANY)
    bf16, f32 = jnp.bfloat16, jnp.float32
    dma = pltpu.SemaphoreType.DMA
    out = pl.pallas_call(
        clip_kernel,
        out_shape=jax.ShapeDtypeStruct((2 * piece, D), bf16),
        in_specs=[vmem, smem, smem] + [vmem] * 8 + [hbm] * 4,
        out_specs=vmem,
        scratch_shapes=[
            pltpu.VMEM(qkv_weight.shape, bf16),
            pltpu.VMEM((LAYERS, D, D), bf16),
            pltpu.VMEM(fc1_weight.shape, bf16),
            pltpu.VMEM(fc2_weight.shape, bf16),
            pltpu.VMEM(fc1_weight.shape, bf16),
            pltpu.VMEM(fc2_weight.shape, bf16),
            pltpu.VMEM(fc1_bias.shape, f32),
            pltpu.VMEM((groups, piece, D), bf16),
            pltpu.VMEM((half, piece, D), bf16),
            pltpu.VMEM((rows, D), f32),
            pltpu.VMEM((rows, D), f32),
            pltpu.VMEM((LAYERS, 2, rows, D), bf16),
            pltpu.VMEM((chunk, D), bf16),
            pltpu.VMEM((2 * rows, width), bf16),
            pltpu.VMEM((2 * rows, width), bf16),
            pltpu.VMEM((2 * rows, width), bf16),
            pltpu.VMEM((2 * rows, 2 * rows), f32),
            pltpu.VMEM((LAYERS, tensor_size, rows, width), bf16),
            pltpu.VMEM((LAYERS, rows, width), bf16),
            pltpu.VMEM((chunk, hidden), bf16),
            pltpu.VMEM((LAYERS, rows, D), bf16),
            pltpu.VMEM((LAYERS, rows, D), bf16),
            pltpu.VMEM((half, piece, D), bf16),
            pltpu.VMEM((2, piece, D), bf16),
            dma((LAYERS, 4)),
            dma((half,)),
            dma((half,)),
            dma((half,)),
            dma((half,)),
            dma((1,)),
            dma((1,)),
            dma((1,)),
            dma((LAYERS, 5 * (half + 1))),
            dma((LAYERS, 5 * (half + 1))),
            dma((LAYERS, SPREAD + 2 * half)),
            dma((LAYERS, SPREAD + 2 * half)),
            dma((half,)),
            dma((2,)),
        ],
        compiler_params=pltpu.CompilerParams(
            collective_id=0, has_side_effects=True, vmem_limit_bytes=60 * 1024 * 1024
        ),
    )(
        frames_in[0],
        frame_time,
        cond_count,
        ln1_gain,
        ln1_bias,
        qkv_bias.transpose(1, 0, 2),
        out_bias,
        ln2_gain,
        ln2_bias,
        fc1_bias,
        fc2_bias,
        qkv_weight,
        out_weight,
        fc1_weight,
        fc2_weight,
    )
    return out[None]


def shards(frames_in, frame_time, cond_count, *rest):
    groups = lax.axis_size("tm")
    seq_count = frames_in.shape[1] // (PATCH_DEV + COND)
    by_clip = frame_time.shape[0] == groups and seq_count == groups
    by_clip = by_clip and lax.axis_size("tensor") == 4 and groups == 8
    body = shards_clip if by_clip else shards_gather
    return body(frames_in, frame_time, cond_count, *rest)


def solution(mesh):
    in_specs = (
        P("tm", None, None),
        P(),
        P(),
        P(),
        P(),
        P(None, None, None, "tensor"),
        P(None, None, "tensor"),
        P(None, "tensor", None),
        P(),
        P(),
        P(),
        P(None, None, "tensor"),
        P(None, "tensor"),
        P(None, "tensor", None),
        P(),
    )
    out_specs = P("tm", "tensor", None)
    return jax.shard_map(shards, mesh=mesh, in_specs=in_specs, out_specs=out_specs, check_vma=False)
```

```python
import jax
import jax.numpy as jnp
from jax import lax
from jax.experimental import pallas as pl
from jax.experimental.pallas import tpu as pltpu
from jax.sharding import PartitionSpec as P

D = 1024
HEADS = 16
PATCH_DEV = 64
COND = 2
LAYERS = 2


def layer_norm(inputs, gain_row, bias_row):
    center = jnp.mean(inputs, axis=-1, keepdims=True)
    spread = jnp.mean(jnp.square(inputs - center), axis=-1, keepdims=True)
    return (inputs - center) * lax.rsqrt(spread + 1e-06) * gain_row + bias_row


def piece_tables(frame_time, cond_count, piece_count, frame_split, piece_rows):
    cond_dev = COND // frame_split
    piece_ids = jnp.arange(piece_count, dtype=jnp.int32)
    frame_ids = jnp.arange(frame_time.shape[0], dtype=jnp.int32)
    matches = (piece_ids // frame_split)[:, None] == frame_ids[None, :]
    piece_time = jnp.sum(jnp.where(matches, frame_time[None, :], 0), axis=1)
    piece_cond = jnp.sum(jnp.where(matches, cond_count[None, :], 0), axis=1)
    slot_index = jnp.arange(piece_rows, dtype=jnp.int32)
    cond_slot = (piece_ids % frame_split)[:, None] * cond_dev + slot_index[None, :] - PATCH_DEV
    valid = (slot_index[None, :] < PATCH_DEV) | (cond_slot < piece_cond[:, None])
    return (piece_time, valid)


def shards_gather(
    frames_in,
    frame_time,
    cond_count,
    ln1_gain,
    ln1_bias,
    qkv_weight,
    qkv_bias,
    out_weight,
    out_bias,
    ln2_gain,
    ln2_bias,
    fc1_weight,
    fc1_bias,
    fc2_weight,
    fc2_bias,
):
    frame_count = frame_time.shape[0]
    piece_count = lax.axis_size("tm")
    frame_split = piece_count // frame_count
    cond_dev = COND // frame_split
    piece_rows = PATCH_DEV + cond_dev
    row_count = frames_in.shape[1]
    seq_count = row_count // piece_rows
    head_dim = D // HEADS
    head_local = qkv_weight.shape[3] // head_dim
    scale = head_dim ** (-0.5)
    tensor_size = lax.axis_size("tensor")
    tensor_pos = lax.axis_index("tensor")
    my_piece = lax.axis_index("tm")
    share_rows = row_count // tensor_size
    piece_time, valid = piece_tables(frame_time, cond_count, piece_count, frame_split, piece_rows)
    piece_ids = jnp.arange(piece_count, dtype=jnp.int32)
    my_time = jnp.sum(jnp.where(piece_ids == my_piece, piece_time, 0))
    full_in = frames_in[0]
    new_share = None
    for layer_idx in range(LAYERS):
        normed = layer_norm(
            full_in.astype(jnp.float32), ln1_gain[layer_idx], ln1_bias[layer_idx]
        ).astype(jnp.bfloat16)
        projected = jnp.einsum(
            "rd,jde->jre", normed, qkv_weight[layer_idx], preferred_element_type=jnp.float32
        )
        projected = (projected + qkv_bias[layer_idx][:, None, :]).astype(jnp.bfloat16)
        queries = projected[0].reshape(seq_count, piece_rows, head_local, head_dim)
        keys_mine = projected[1].reshape(1, seq_count, piece_rows, head_local * head_dim)
        values_mine = projected[2].reshape(1, seq_count, piece_rows, head_local * head_dim)
        start_top = jnp.full((seq_count, head_local, piece_rows), -1e30, jnp.float32)
        key_block = lax.all_gather(keys_mine, "tm", axis=0, tiled=True)
        value_block = lax.all_gather(values_mine, "tm", axis=0, tiled=True)
        block_count = key_block.shape[0]
        block_ids = jnp.arange(block_count, dtype=jnp.int32)
        matches = block_ids[:, None] == piece_ids[None, :]
        key_time = jnp.sum(jnp.where(matches, piece_time[None, :], 0), axis=1)
        key_valid = jnp.any(matches[:, :, None] & valid[None, :, :], axis=1)
        allowed = (key_time <= my_time)[:, None] & key_valid
        top_run = start_top
        keys_split = key_block.reshape(block_count, seq_count, piece_rows, head_local, head_dim)
        values_split = value_block.reshape(block_count, seq_count, piece_rows, head_local, head_dim)
        scores = (
            jnp.einsum("sqhd,gskhd->shqgk", queries, keys_split, preferred_element_type=jnp.float32)
            * scale
        )
        scores = jnp.where(allowed, scores, -1e30)
        new_top = jnp.maximum(top_run, jnp.max(scores, axis=(3, 4)))
        weights = jnp.where(allowed, jnp.exp(scores - new_top[..., None, None]), 0.0)
        total_new = jnp.sum(weights, axis=(3, 4))
        mixed = jnp.einsum(
            "shqgk,gskhd->shqd",
            weights.astype(jnp.bfloat16),
            values_split,
            preferred_element_type=jnp.float32,
        )
        top_run = new_top
        attended = (
            (mixed / total_new[..., None])
            .transpose(0, 2, 1, 3)
            .reshape(row_count, head_local * head_dim)
            .astype(jnp.bfloat16)
        )
        out_layer = out_weight[layer_idx]
        fc1_layer = fc1_weight[layer_idx]
        fc2_layer = fc2_weight[layer_idx]
        fc1_layer_bias = fc1_bias[layer_idx]
        own_rows = lax.dynamic_slice_in_dim(full_in, tensor_pos * share_rows, share_rows, 0).astype(
            jnp.float32
        )
        first = (
            own_rows
            + lax.psum_scatter(
                jnp.dot(attended, out_layer, preferred_element_type=jnp.float32).astype(
                    jnp.bfloat16
                ),
                "tensor",
                scatter_dimension=0,
                tiled=True,
            ).astype(jnp.float32)
            + out_bias[layer_idx]
        )
        normed_two = layer_norm(first, ln2_gain[layer_idx], ln2_bias[layer_idx]).astype(
            jnp.bfloat16
        )
        inner = jax.nn.gelu(
            jnp.dot(
                lax.all_gather(normed_two, "tensor", axis=0, tiled=True),
                fc1_layer,
                preferred_element_type=jnp.float32,
            )
            + fc1_layer_bias,
            approximate=False,
        ).astype(jnp.bfloat16)
        mlp_share = lax.psum_scatter(
            jnp.dot(inner, fc2_layer, preferred_element_type=jnp.float32).astype(jnp.bfloat16),
            "tensor",
            scatter_dimension=0,
            tiled=True,
        ).astype(jnp.float32)
        new_share = (first + mlp_share + fc2_bias[layer_idx]).astype(jnp.bfloat16)
        if layer_idx + 1 < LAYERS:
            full_in = lax.all_gather(new_share, "tensor", axis=0, tiled=True)
    return new_share[None]


MESH = pl.DeviceIdType.MESH
FAR = 1 << 30
N1, AP, AD, AO, XS = range(5)
OWN, PIECE, REST, UP, DOWN, SPREAD = range(6)


def clip_kernel(
    x_ref, time_ref, cond_ref, g1, b1, qkvb, ob, g2, b2, f1b, f2b, wqkv_h, wo_h, w1_h, w2_h,
    out_ref, wqkv, wo, w1, w2, w1p, w2p, f1p, blk_s, cnd_s, blk_r, cnd_r, xs, keep, nrm1, nrm2, qb, kb, vb, mask,
    att, att_p, inner, us, ur, out_s, out_r, ocn_s, ocn_r,
    wsem, in_s, in_r, fw_s, fw_r, loc, bs, br, ls, lr, ws, wr, os, orr,
):
    groups = blk_s.shape[0]
    half = blk_r.shape[0]
    patch = PATCH_DEV
    piece = patch + COND
    rows = xs.shape[0]
    lead = rows - half * patch
    chunks = [(lead + i * patch, patch) for i in range(half)]
    chunks[0] = (0, lead + patch)
    cut = lead + (half // 2) * patch
    spans = ((0, cut), (cut, rows - cut))
    per = half // 2
    head_dim = D // HEADS
    width = qb.shape[1]
    head_local = width // head_dim
    share = width // groups
    last = LAYERS - 1

    t = lax.axis_index("tm")
    me = lax.axis_index("tensor")
    x = me // 2
    c = me % 2
    partner = me + 1 - 2 * c
    beside = t + 1 - 2 * (t % 2)
    across = (me + 2) % 4
    diagonal = (partner + 2) % 4

    def clip_of(g):
        return g // 2 + half * ((g // 2 + g) % 2)

    def group_of(clip):
        z = clip % half
        return 2 * z + (clip // half + z) % 2

    clip = clip_of(t)
    goal_x = clip // half
    goal = clip // 2

    pairs = ((wqkv_h, wqkv), (wo_h, wo), (w1_h, w1), (w2_h, w2))

    def weight_copy(l, j):
        dst = pairs[j][1].at[l]
        if j == 1:
            dst = wo.at[l, pl.ds(pl.multiple_of(me * width, width), width)]
        return pltpu.make_async_copy(pairs[j][0].at[l], dst, wsem.at[l, j])

    for l in range(LAYERS):
        for j in ((1, 0, 2, 3) if l == 0 else (0, 1, 2, 3)):
            weight_copy(l, j).start()

    def remote(src, dst, s, r, to):
        return pltpu.make_async_remote_copy(
            src_ref=src, dst_ref=dst, send_sem=s, recv_sem=r, device_id=to, device_id_type=MESH
        )

    barrier = pltpu.get_barrier_semaphore()

    def hello(g, j):
        pl.semaphore_signal(barrier, inc=1, device_id=(g, j), device_id_type=MESH)

    for other in (partner, across, diagonal):
        hello(t, other)
    for d in range(1, groups):
        hello((t + d) % groups, me)
    for s in range(2):
        g = group_of(2 * me + s)
        j = x * 2 + t // half

        @pl.when(jnp.logical_or(g != t, j != me))
        def _():
            hello(g, j)

    for g in range(groups):
        blk_s[g] = x_ref[g * piece : g * piece + patch]
        cnd_s[g] = x_ref[g * piece + patch : (g + 1) * piece]

    home = c == t // half
    own_copies = [
        pltpu.make_async_copy(src.at[clip], dst.at[t % half], loc.at[j])
        for j, (src, dst) in enumerate(((blk_s, blk_r), (cnd_s, cnd_r)))
    ]

    @pl.when(home)
    def _():
        for copy in own_copies:
            copy.start()

    def times(axis, query):
        shape = (2 * rows, 1) if axis == 0 else (1, 2 * rows)
        at = lax.broadcasted_iota(jnp.int32, shape, axis)
        out = jnp.full(shape, FAR // 2 if query else FAR, jnp.int32)
        for f in range(groups):
            base = (f // half) * rows
            lo = base + lead + (f % half) * patch
            out = jnp.where((at >= lo) & (at < lo + patch), time_ref[f], out)
            lo = base + COND * (f % half)
            hi = lo + (COND if query else cond_ref[f])
            out = jnp.where((at >= lo) & (at < hi), time_ref[f], out)
        return out

    mask[...] = jnp.where(times(1, False) <= times(0, True), 0.0, -1e30)
    xs[0:lead] = jnp.zeros((lead, D), jnp.float32)

    targets = jnp.where(x == goal_x, half, 0)
    targets = targets - jnp.where((x == goal_x) & (goal == me) & home, 1, 0)
    with jax.named_scope("barrier"):
        pl.semaphore_wait(barrier, 3 + groups - 1 + targets)

    def enter(i, j):
        far = jnp.where(x == 0, t // 2 + 2, half - 1 - t // 2)
        z = (far + 2 * (i // 2)) % half
        g = 2 * z + (i + t) % 2
        k = t % half
        src, dst = ((blk_s, blk_r), (cnd_s, cnd_r))[j]
        return g, remote(src.at[clip_of(g)], dst.at[k], in_s.at[j, i], in_r.at[j, k], (g, me))

    for j in range(2):
        for i in range(half):
            g, copy = enter(i, j)

            @pl.when(home & (g != t))
            def _():
                copy.start()

    def span(j, first, count):
        return pl.ds(pl.multiple_of(j * width + first, share), count)

    def wo_own(l):
        at = wo.at[l, span(me, 0, width)]
        return remote(at, at, ws.at[l, OWN], wr.at[l, OWN], (t, partner))

    def wo_piece(l):
        at = wo.at[l, span(me, share * t, share)]
        return remote(at, at, ws.at[l, PIECE], wr.at[l, PIECE], (t, across))

    def wo_slice(l, g):
        return wo.at[l, span(across, share * g, share)]

    def wo_column(l, d, g):
        at = wo_slice(l, g)
        to = (t + 2 * d) % groups
        return remote(at, at, ws.at[l, SPREAD + d], wr.at[l, SPREAD + d], (to, me))

    def wo_row(l, d, g):
        at = wo_slice(l, g)
        j = SPREAD + half + d
        return remote(at, at, ws.at[l, j], wr.at[l, j], (beside, me))

    def wo_rest(l):
        at = wo.at[l, span(across, 0, width)]
        return remote(at, at, ws.at[l, REST], wr.at[l, REST], (t, partner))

    def mlp_weights(l):
        return [
            remote(src.at[l], dst.at[l], ws.at[l, j], wr.at[l, j], (t, partner))
            for j, src, dst in ((UP, w1_h, w1p), (DOWN, w2_h, w2p))
        ]

    def wo_begin(l):
        weight_copy(l, 1).wait()
        wo_piece(l).start()
        wo_own(l).start()

    def wo_share(l):
        wo_piece(l).wait_recv()
        for d in range(1, half):
            wo_column(l, d, t).start()
        wo_row(l, 0, t).start()

    def wo_relay(l, d):
        g = (t - 2 * d + groups) % groups
        wo_column(l, d, g).wait_recv()
        wo_row(l, d, g).start()

    def wo_finish(l):
        for d in range(half):
            wo_row(l, d, (beside - 2 * d + groups) % groups).wait_recv()
        wo_rest(l).start()

    bias_copy = remote(f1b, f1p, bs.at[0], br.at[0], (t, partner))
    wo_begin(0)
    bias_copy.start()
    for copy in mlp_weights(0):
        copy.start()

    def onward(k, j=0):
        at = (blk_r, cnd_r)[j].at[k]
        return remote(at, at, fw_s.at[j, k], fw_r.at[j, k], (t, across))

    def arrival(k, j=0):
        src, dst = ((blk_s, blk_r), (cnd_s, cnd_r))[j]
        return remote(src.at[0], dst.at[k], in_s.at[j, 0], in_r.at[j, k], (t, across))

    first_k = per * ((t // 2 + x) % 2)
    with jax.named_scope("wo_first"):
        wo_share(0)

    def near(i):
        return first_k + (i + t) % 2

    def cross(i):
        return per - first_k + (i + t) % 2

    for i in range(per):
        k = near(i)

        @pl.when(half * c + k != t)
        def _():
            with jax.named_scope("in_direct"):
                arrival(k).wait_recv()
            onward(k).start()

    def norm(v, gain, bias):
        return layer_norm(v, gain, bias).astype(jnp.bfloat16)

    def in_half(h, r0, count):
        return pl.ds(pl.multiple_of(h * rows + r0, 16), count)

    def ids(l, kind, i):
        return ls.at[l, kind * (half + 1) + i], lr.at[l, kind * (half + 1) + i]

    def normed_send(l, i):
        at = nrm1.at[l, c, pl.ds(*chunks[i])]
        return remote(at, at, *ids(l, N1, i), (t, partner))

    def normed_come(l, i):
        at = nrm1.at[l, 1 - c, pl.ds(*chunks[i])]
        return remote(at, at, *ids(l, N1, i), (t, partner))

    def att_send(l, i, kind):
        at = pl.ds(*spans[i])
        to = {AP: partner, AD: diagonal, AO: across}[kind]
        src = att.at[l, me, at] if kind == AO else att_p.at[l, at]
        return remote(src, att.at[l, me, at], *ids(l, kind, i), (t, to))

    def att_come(l, i, kind):
        to = {AP: partner, AD: diagonal, AO: across}[kind]
        dst = att.at[l, to, pl.ds(*spans[i])]
        return remote(dst, dst, *ids(l, kind, i), (t, to))

    def cross_send(l, i):
        at = pl.ds(*chunks[i])
        return remote(us.at[l, at], ur.at[l, at], *ids(l, XS, i), (t, across))

    def leave(k, j=0):
        src, dst = ((out_s, out_r), (ocn_s, ocn_r))[j]
        s = clip % 2
        return remote(src.at[k], dst.at[s], os.at[j, k], orr.at[j, s], (half * c + k, goal))

    def stay(k, j=0):
        src, dst = ((out_s, out_r), (ocn_s, ocn_r))[j]
        return pltpu.make_async_copy(src.at[k], dst.at[clip % 2], orr.at[j, clip % 2])

    def depart(k, j=0):
        here = (half * c + k == t) & (goal == me)

        @pl.when(here)
        def _():
            stay(k, j).start()

        @pl.when(jnp.logical_not(here))
        def _():
            leave(k, j).start()

    def project(l, h, r0, m):
        at = pl.ds(r0 if isinstance(r0, int) else pl.multiple_of(r0, 16), m)
        normed = nrm1[l, h, at]
        for j, dst in enumerate((qb, kb, vb)):
            y = jnp.dot(normed, wqkv[l, j], preferred_element_type=jnp.float32)
            y = y + qkvb[j, pl.ds(l, 1)]
            if j == 0:
                y = y * head_dim ** (-0.5)
            dst[in_half(h, r0, m)] = y.astype(jnp.bfloat16)

    def strip(i):
        return pl.ds(pl.multiple_of(lead + i * patch, 16), patch) if i is not None else pl.ds(0, lead)

    def block_send(h, i):
        at = nrm1.at[0, h, strip(i)]
        return remote(at, at, *ids(0, N1, half if i is None else i), (t, partner))

    def normed_in(i):
        at = strip(i)
        nrm1[0, c, at] = norm(xs[at], g1[0:1], b1[0:1])
        block_send(c, i).start()

    def take(k):
        xs[strip(k)] = blk_r[k].astype(jnp.float32)
        normed_in(k)
        project(0, c, lead + k * patch, patch)

    def take_other(k):
        with jax.named_scope("n1_wait"):
            block_send(1 - c, k).wait_recv()
        project(0, 1 - c, lead + k * patch, patch)

    def local(k):
        @pl.when(half * c + k == t)
        def _():
            own_copies[0].wait()

    def relay(d):
        with jax.named_scope("wo_relay"):
            wo_relay(0, d)

    weight_copy(0, 0).wait()
    for i in range(per):
        local(near(i))
        take(near(i))
    relay(1)
    for i in range(per):
        k = cross(i)
        local(k)

        @pl.when(half * c + k != t)
        def _():
            with jax.named_scope("in_cross"):
                onward(k).wait_recv()

        take(k)
        if i == 0:
            for j in range(per):
                k = near(j)

                @pl.when(half * c + k != t)
                def _():
                    arrival(k, 1).wait_recv()
                    onward(k, 1).start()

        take_other(near(i))
        relay(2 + i)
    for i in range(per):
        k = cross(i)

        @pl.when(half * c + k != t)
        def _():
            onward(k, 1).wait_recv()

    @pl.when(home)
    def _():
        own_copies[1].wait()

    for k in range(half):
        xs[COND * k : COND * (k + 1)] = cnd_r[k].astype(jnp.float32)
    normed_in(None)
    for l in range(1, LAYERS):
        wo_begin(l)
    project(0, c, 0, lead)
    for i in range(per):
        take_other(cross(i))
    block_send(1 - c, None).wait_recv()
    project(0, 1 - c, 0, lead)

    lane = lax.broadcasted_iota(jnp.int32, (1, width), 1)
    heads = [(lane >= h * head_dim) & (lane < (h + 1) * head_dim) for h in range(head_local)]

    def layer(l, carry):
        def attend(h, r0, m):
            q = qb[in_half(h, r0, m)]
            stacked = jnp.concatenate(
                [q * jnp.where(on, 1.0, 0.0).astype(jnp.bfloat16) for on in heads], axis=0
            )
            sc = lax.dot_general(
                stacked, kb[...], (((1,), (1,)), ((), ())), preferred_element_type=jnp.float32
            )
            hide = mask[in_half(h, r0, m)]
            parts, totals = [], []
            for j in range(head_local):
                s = sc[j * m : (j + 1) * m] + hide
                w = jnp.exp(s - jnp.max(s, axis=-1, keepdims=True))
                totals.append(jnp.sum(w, axis=-1, keepdims=True))
                parts.append(w.astype(jnp.bfloat16))
            pv = jnp.dot(
                jnp.concatenate(parts, axis=0), vb[...], preferred_element_type=jnp.float32
            )
            acc = jnp.zeros((m, width), jnp.float32)
            for j in range(head_local):
                acc = jnp.where(heads[j], pv[j * m : (j + 1) * m] * (1.0 / totals[j]), acc)
            return acc.astype(jnp.bfloat16)

        for i, (r0, m) in enumerate(spans):
            with jax.named_scope("attend_other"):
                att_p[l, r0 : r0 + m] = attend(1 - c, r0, m)
            att_send(l, i, AD).start()
            att_send(l, i, AP).start()
            with jax.named_scope("attend_own"):
                att[l, me, r0 : r0 + m] = attend(c, r0, m)
            att_send(l, i, AO).start()
            if i == 0:
                with jax.named_scope("wo_finish"):
                    wo_finish(l)

        @pl.when(l < last)
        def _():
            for copy in mlp_weights(l + 1):
                copy.start()

        with jax.named_scope("wo_rest_wait"):
            wo_own(l).wait_recv()
            wo_rest(l).wait_recv()
        weight_copy(l, 2).wait()
        weight_copy(l, 3).wait()

        def ready(i, r0, m):
            with jax.named_scope("att_wait"):
                for kind in (AP, AD, AO):
                    att_come(l, i, kind).wait_recv()
            full = jnp.concatenate([att[l, j, r0 : r0 + m] for j in range(4)], axis=1)
            first = jnp.dot(full, wo[l], preferred_element_type=jnp.float32)
            first = xs[r0 : r0 + m] + first + ob[pl.ds(l, 1)]
            xs[r0 : r0 + m] = first
            nrm2[0:m] = norm(first, g2[pl.ds(l, 1)], b2[pl.ds(l, 1)])

        def mlp(m):
            tile = 256
            hidden = w1.shape[2]
            total = 0.0
            for p, (up, bias, down) in enumerate(((w1, f1b, w2), (w1p, f1p, w2p))):
                for n in range(hidden // tile):
                    at = pl.ds(n * tile, tile)
                    y = jnp.dot(nrm2[0:m], up[l, :, at], preferred_element_type=jnp.float32)
                    y = y + bias[pl.ds(l, 1), at]
                    y = 0.5 * y * (1.0 + lax.erf(y * (0.5**0.5)))
                    inner[0:m, pl.ds(n * tile, tile)] = y.astype(jnp.bfloat16)
                total = total + jnp.dot(
                    inner[0:m], down[l], preferred_element_type=jnp.float32
                )
            return total

        sends_x = jnp.logical_or(l < last, x != goal_x)
        takes_x = jnp.logical_or(l < last, x == goal_x)

        for i, (r0, m) in enumerate(spans):
            ready(i, r0, m)
            if i == 0:
                with jax.named_scope("weights_wait"):

                    @pl.when(l == 0)
                    def _():
                        bias_copy.wait_recv()

                    for copy in mlp_weights(l):
                        copy.wait_recv()
            with jax.named_scope("mlp"):
                u = mlp(m)
                keep[r0 : r0 + m] = u
                us[l, r0 : r0 + m] = u.astype(jnp.bfloat16)

            @pl.when(sends_x)
            def _():
                for j in range(per * i, per * (i + 1)):
                    cross_send(l, j).start()

            if i == 0:

                @pl.when(l < last)
                def _():
                    wo_share(l + 1)

        @pl.when(l < last)
        def _():
            weight_copy(l + 1, 0).wait()

        def other(i):
            with jax.named_scope("n1_wait"):
                normed_come(l + 1, i).wait_recv()
            project(l + 1, 1 - c, *chunks[i])

        for i, (r0, m) in enumerate(chunks):

            @pl.when(takes_x)
            def _():
                with jax.named_scope("x_wait"):
                    cross_send(l, i).wait_recv()
                new = xs[r0 : r0 + m] + keep[r0 : r0 + m] + f2b[pl.ds(l, 1)]
                new = (new + ur[l, r0 : r0 + m].astype(jnp.float32)).astype(jnp.bfloat16)

                @pl.when(l < last)
                def _():
                    wide = new.astype(jnp.float32)
                    xs[r0 : r0 + m] = wide
                    nrm1[l + 1, c, r0 : r0 + m] = norm(
                        wide, g1[pl.ds(l + 1, 1)], b1[pl.ds(l + 1, 1)]
                    )
                    normed_send(l + 1, i).start()
                    project(l + 1, c, r0, m)
                    if i > 0:
                        other(i - 1)

                @pl.when(l == last)
                def _():
                    out_s[i] = new[m - patch :]
                    depart(i)
                    if i == 0:
                        for k in range(half):
                            ocn_s[k] = new[COND * k : COND * (k + 1)]
                            depart(k, 1)

            if i == half - 3:

                @pl.when(l < last)
                def _():
                    with jax.named_scope("wo_relay"):
                        for d in range(1, half):
                            wo_relay(l + 1, d)

        @pl.when(l < last)
        def _():
            other(half - 1)

        return carry

    lax.fori_loop(0, LAYERS, layer, 0)

    for i in range(half):
        for j in range(2):
            g, copy = enter(i, j)

            @pl.when(home & (g != t))
            def _():
                copy.wait_send()

    for i in range(per):
        k = near(i)

        @pl.when(half * c + k != t)
        def _():
            for j in range(2):
                onward(k, j).wait_send()

    bias_copy.wait_send()
    for i in range(half):
        block_send(c, i).wait_send()
    block_send(c, None).wait_send()

    def drain(l, carry):
        for i in range(half):

            @pl.when(l > 0)
            def _():
                normed_send(l, i).wait_send()

            @pl.when(jnp.logical_or(l < last, x != goal_x))
            def _():
                cross_send(l, i).wait_send()

        for i in range(len(spans)):
            for kind in (AP, AD, AO):
                att_send(l, i, kind).wait_send()

        wo_own(l).wait_send()
        wo_piece(l).wait_send()
        wo_rest(l).wait_send()
        for d in range(1, half):
            wo_column(l, d, t).wait_send()
        for d in range(half):
            wo_row(l, d, t).wait_send()
        for copy in mlp_weights(l):
            copy.wait_send()
        return carry

    lax.fori_loop(0, LAYERS, drain, 0)

    for k in range(half):
        here = (half * c + k == t) & (goal == me)

        @pl.when((x == goal_x) & jnp.logical_not(here))
        def _():
            for j in range(2):
                leave(k, j).wait_send()

    for s in range(2):
        there = 2 * me + s
        here = (group_of(there) == t) & (x * 2 + t // half == me)

        @pl.when(here)
        def _():
            for j, (src, dst) in enumerate(((out_s, out_r), (ocn_s, ocn_r))):
                pltpu.make_async_copy(src.at[t % half], dst.at[s], orr.at[j, s]).wait()

        @pl.when(jnp.logical_not(here))
        def _():
            with jax.named_scope("out_wait"):
                for j, (src, dst) in enumerate(((out_s, out_r), (ocn_s, ocn_r))):
                    remote(
                        src.at[0], dst.at[s], os.at[j, 0], orr.at[j, s], (t, across)
                    ).wait_recv()

        out_ref[s * piece : s * piece + patch] = out_r[s]
        out_ref[s * piece + patch : (s + 1) * piece] = ocn_r[s]


def shards_clip(
    frames_in,
    frame_time,
    cond_count,
    ln1_gain,
    ln1_bias,
    qkv_weight,
    qkv_bias,
    out_weight,
    out_bias,
    ln2_gain,
    ln2_bias,
    fc1_weight,
    fc1_bias,
    fc2_weight,
    fc2_bias,
):
    groups = lax.axis_size("tm")
    tensor_size = lax.axis_size("tensor")
    piece = PATCH_DEV + COND
    half = groups // 2
    width = qkv_weight.shape[3]
    hidden = fc1_weight.shape[2]
    lead = -(-half * COND // 16) * 16
    rows = lead + half * PATCH_DEV
    chunk = lead + (half // 2) * PATCH_DEV

    vmem = pl.BlockSpec(memory_space=pltpu.VMEM)
    smem = pl.BlockSpec(memory_space=pltpu.SMEM)
    hbm = pl.BlockSpec(memory_space=pl.ANY)
    bf16, f32 = jnp.bfloat16, jnp.float32
    dma = pltpu.SemaphoreType.DMA
    out = pl.pallas_call(
        clip_kernel,
        out_shape=jax.ShapeDtypeStruct((2 * piece, D), bf16),
        in_specs=[vmem, smem, smem] + [vmem] * 8 + [hbm] * 4,
        out_specs=vmem,
        scratch_shapes=[
            pltpu.VMEM(qkv_weight.shape, bf16),
            pltpu.VMEM((LAYERS, D, D), bf16),
            pltpu.VMEM(fc1_weight.shape, bf16),
            pltpu.VMEM(fc2_weight.shape, bf16),
            pltpu.VMEM(fc1_weight.shape, bf16),
            pltpu.VMEM(fc2_weight.shape, bf16),
            pltpu.VMEM(fc1_bias.shape, f32),
            pltpu.VMEM((groups, PATCH_DEV, D), bf16),
            pltpu.VMEM((groups, COND, D), bf16),
            pltpu.VMEM((half, PATCH_DEV, D), bf16),
            pltpu.VMEM((half, COND, D), bf16),
            pltpu.VMEM((rows, D), f32),
            pltpu.VMEM((rows, D), f32),
            pltpu.VMEM((LAYERS, 2, rows, D), bf16),
            pltpu.VMEM((chunk, D), bf16),
            pltpu.VMEM((2 * rows, width), bf16),
            pltpu.VMEM((2 * rows, width), bf16),
            pltpu.VMEM((2 * rows, width), bf16),
            pltpu.VMEM((2 * rows, 2 * rows), f32),
            pltpu.VMEM((LAYERS, tensor_size, rows, width), bf16),
            pltpu.VMEM((LAYERS, rows, width), bf16),
            pltpu.VMEM((chunk, hidden), bf16),
            pltpu.VMEM((LAYERS, rows, D), bf16),
            pltpu.VMEM((LAYERS, rows, D), bf16),
            pltpu.VMEM((half, PATCH_DEV, D), bf16),
            pltpu.VMEM((2, PATCH_DEV, D), bf16),
            pltpu.VMEM((half, COND, D), bf16),
            pltpu.VMEM((2, COND, D), bf16),
            dma((LAYERS, 4)),
            dma((2, half)),
            dma((2, half)),
            dma((2, half)),
            dma((2, half)),
            dma((2,)),
            dma((1,)),
            dma((1,)),
            dma((LAYERS, 5 * (half + 1))),
            dma((LAYERS, 5 * (half + 1))),
            dma((LAYERS, SPREAD + 2 * half)),
            dma((LAYERS, SPREAD + 2 * half)),
            dma((2, half)),
            dma((2, 2)),
        ],
        compiler_params=pltpu.CompilerParams(
            collective_id=0, has_side_effects=True, vmem_limit_bytes=60 * 1024 * 1024
        ),
    )(
        frames_in[0],
        frame_time,
        cond_count,
        ln1_gain,
        ln1_bias,
        qkv_bias.transpose(1, 0, 2),
        out_bias,
        ln2_gain,
        ln2_bias,
        fc1_bias,
        fc2_bias,
        qkv_weight,
        out_weight,
        fc1_weight,
        fc2_weight,
    )
    return out[None]


def shards(frames_in, frame_time, cond_count, *rest):
    groups = lax.axis_size("tm")
    seq_count = frames_in.shape[1] // (PATCH_DEV + COND)
    by_clip = frame_time.shape[0] == groups and seq_count == groups
    by_clip = by_clip and lax.axis_size("tensor") == 4 and groups == 8
    body = shards_clip if by_clip else shards_gather
    return body(frames_in, frame_time, cond_count, *rest)


def solution(mesh):
    in_specs = (
        P("tm", None, None),
        P(),
        P(),
        P(),
        P(),
        P(None, None, None, "tensor"),
        P(None, None, "tensor"),
        P(None, "tensor", None),
        P(),
        P(),
        P(),
        P(None, None, "tensor"),
        P(None, "tensor"),
        P(None, "tensor", None),
        P(),
    )
    out_specs = P("tm", "tensor", None)
    return jax.shard_map(shards, mesh=mesh, in_specs=in_specs, out_specs=out_specs, check_vma=False)
```

```python
import jax
import jax.numpy as jnp
from jax import lax
from jax.experimental import pallas as pl
from jax.experimental.pallas import tpu as pltpu
from jax.sharding import PartitionSpec as P

D = 1024
HEADS = 16
PATCH_DEV = 64
COND = 2
LAYERS = 2


def layer_norm(inputs, gain_row, bias_row):
    center = jnp.mean(inputs, axis=-1, keepdims=True)
    spread = jnp.mean(jnp.square(inputs - center), axis=-1, keepdims=True)
    return (inputs - center) * lax.rsqrt(spread + 1e-06) * gain_row + bias_row


def piece_tables(frame_time, cond_count, piece_count, frame_split, piece_rows):
    cond_dev = COND // frame_split
    piece_ids = jnp.arange(piece_count, dtype=jnp.int32)
    frame_ids = jnp.arange(frame_time.shape[0], dtype=jnp.int32)
    matches = (piece_ids // frame_split)[:, None] == frame_ids[None, :]
    piece_time = jnp.sum(jnp.where(matches, frame_time[None, :], 0), axis=1)
    piece_cond = jnp.sum(jnp.where(matches, cond_count[None, :], 0), axis=1)
    slot_index = jnp.arange(piece_rows, dtype=jnp.int32)
    cond_slot = (piece_ids % frame_split)[:, None] * cond_dev + slot_index[None, :] - PATCH_DEV
    valid = (slot_index[None, :] < PATCH_DEV) | (cond_slot < piece_cond[:, None])
    return (piece_time, valid)


def shards_gather(
    frames_in,
    frame_time,
    cond_count,
    ln1_gain,
    ln1_bias,
    qkv_weight,
    qkv_bias,
    out_weight,
    out_bias,
    ln2_gain,
    ln2_bias,
    fc1_weight,
    fc1_bias,
    fc2_weight,
    fc2_bias,
):
    frame_count = frame_time.shape[0]
    piece_count = lax.axis_size("tm")
    frame_split = piece_count // frame_count
    cond_dev = COND // frame_split
    piece_rows = PATCH_DEV + cond_dev
    row_count = frames_in.shape[1]
    seq_count = row_count // piece_rows
    head_dim = D // HEADS
    head_local = qkv_weight.shape[3] // head_dim
    scale = head_dim ** (-0.5)
    tensor_size = lax.axis_size("tensor")
    tensor_pos = lax.axis_index("tensor")
    my_piece = lax.axis_index("tm")
    share_rows = row_count // tensor_size
    piece_time, valid = piece_tables(frame_time, cond_count, piece_count, frame_split, piece_rows)
    piece_ids = jnp.arange(piece_count, dtype=jnp.int32)
    my_time = jnp.sum(jnp.where(piece_ids == my_piece, piece_time, 0))
    full_in = frames_in[0]
    new_share = None
    for layer_idx in range(LAYERS):
        normed = layer_norm(
            full_in.astype(jnp.float32), ln1_gain[layer_idx], ln1_bias[layer_idx]
        ).astype(jnp.bfloat16)
        projected = jnp.einsum(
            "rd,jde->jre", normed, qkv_weight[layer_idx], preferred_element_type=jnp.float32
        )
        projected = (projected + qkv_bias[layer_idx][:, None, :]).astype(jnp.bfloat16)
        queries = projected[0].reshape(seq_count, piece_rows, head_local, head_dim)
        keys_mine = projected[1].reshape(1, seq_count, piece_rows, head_local * head_dim)
        values_mine = projected[2].reshape(1, seq_count, piece_rows, head_local * head_dim)
        start_top = jnp.full((seq_count, head_local, piece_rows), -1e30, jnp.float32)
        key_block = lax.all_gather(keys_mine, "tm", axis=0, tiled=True)
        value_block = lax.all_gather(values_mine, "tm", axis=0, tiled=True)
        block_count = key_block.shape[0]
        block_ids = jnp.arange(block_count, dtype=jnp.int32)
        matches = block_ids[:, None] == piece_ids[None, :]
        key_time = jnp.sum(jnp.where(matches, piece_time[None, :], 0), axis=1)
        key_valid = jnp.any(matches[:, :, None] & valid[None, :, :], axis=1)
        allowed = (key_time <= my_time)[:, None] & key_valid
        top_run = start_top
        keys_split = key_block.reshape(block_count, seq_count, piece_rows, head_local, head_dim)
        values_split = value_block.reshape(block_count, seq_count, piece_rows, head_local, head_dim)
        scores = (
            jnp.einsum("sqhd,gskhd->shqgk", queries, keys_split, preferred_element_type=jnp.float32)
            * scale
        )
        scores = jnp.where(allowed, scores, -1e30)
        new_top = jnp.maximum(top_run, jnp.max(scores, axis=(3, 4)))
        weights = jnp.where(allowed, jnp.exp(scores - new_top[..., None, None]), 0.0)
        total_new = jnp.sum(weights, axis=(3, 4))
        mixed = jnp.einsum(
            "shqgk,gskhd->shqd",
            weights.astype(jnp.bfloat16),
            values_split,
            preferred_element_type=jnp.float32,
        )
        top_run = new_top
        attended = (
            (mixed / total_new[..., None])
            .transpose(0, 2, 1, 3)
            .reshape(row_count, head_local * head_dim)
            .astype(jnp.bfloat16)
        )
        out_layer = out_weight[layer_idx]
        fc1_layer = fc1_weight[layer_idx]
        fc2_layer = fc2_weight[layer_idx]
        fc1_layer_bias = fc1_bias[layer_idx]
        own_rows = lax.dynamic_slice_in_dim(full_in, tensor_pos * share_rows, share_rows, 0).astype(
            jnp.float32
        )
        first = (
            own_rows
            + lax.psum_scatter(
                jnp.dot(attended, out_layer, preferred_element_type=jnp.float32).astype(
                    jnp.bfloat16
                ),
                "tensor",
                scatter_dimension=0,
                tiled=True,
            ).astype(jnp.float32)
            + out_bias[layer_idx]
        )
        normed_two = layer_norm(first, ln2_gain[layer_idx], ln2_bias[layer_idx]).astype(
            jnp.bfloat16
        )
        inner = jax.nn.gelu(
            jnp.dot(
                lax.all_gather(normed_two, "tensor", axis=0, tiled=True),
                fc1_layer,
                preferred_element_type=jnp.float32,
            )
            + fc1_layer_bias,
            approximate=False,
        ).astype(jnp.bfloat16)
        mlp_share = lax.psum_scatter(
            jnp.dot(inner, fc2_layer, preferred_element_type=jnp.float32).astype(jnp.bfloat16),
            "tensor",
            scatter_dimension=0,
            tiled=True,
        ).astype(jnp.float32)
        new_share = (first + mlp_share + fc2_bias[layer_idx]).astype(jnp.bfloat16)
        if layer_idx + 1 < LAYERS:
            full_in = lax.all_gather(new_share, "tensor", axis=0, tiled=True)
    return new_share[None]


MESH = pl.DeviceIdType.MESH
FAR = 1 << 30
N1, AP, AD, AO, XS = range(5)
OWN, PIECE, REST, UP, DOWN, SPREAD = range(6)


def clip_kernel(
    x_h, time_h, cond_h, g1_h, b1_h, qkvb_h, ob_h, g2_h, b2_h, f1b_h, f2b_h, wqkv_h, wo_h, w1_h,
    w2_h, out_ref, x_ref, time_ref, cond_ref, g1, b1, qkvb, ob, g2, b2, f1b, f2b, small, wqkv, wo, w1, w2, w1p, w2p, f1p, blk_s, cnd_s, blk_r, cnd_r, xs, keep, nrm1, nrm2, qb, kb, vb, mask,
    att, att_p, inner, us, ur, out_s, out_r, ocn_s, ocn_r,
    wsem, in_s, in_r, fw_s, fw_r, loc, bs, br, ls, lr, ws, wr, os, orr,
):
    groups = blk_s.shape[0]
    half = blk_r.shape[0]
    patch = PATCH_DEV
    piece = patch + COND
    rows = xs.shape[0]
    lead = rows - half * patch
    chunks = [(lead + i * patch, patch) for i in range(half)]
    chunks[0] = (0, lead + patch)
    per = half // 2
    members = [[i] for i in range(per)] + [list(range(per, half))]
    spans = [(chunks[g[0]][0], sum(chunks[i][1] for i in g)) for g in members]
    head_dim = D // HEADS
    width = qb.shape[1]
    head_local = width // head_dim
    share = width // groups
    last = LAYERS - 1

    t = lax.axis_index("tm")
    me = lax.axis_index("tensor")
    x = me // 2
    c = me % 2
    mine = (c + t // half) % 2
    partner = me + 1 - 2 * c
    beside = t + 1 - 2 * (t % 2)
    across = (me + 2) % 4
    diagonal = (partner + 2) % 4

    def clip_of(g):
        return g // 2 + half * ((g // 2 + g) % 2)

    def group_of(clip):
        z = clip % half
        return 2 * z + (clip // half + z) % 2

    clip = clip_of(t)
    goal_x = clip // half
    goal = clip // 2

    pairs = ((wqkv_h, wqkv), (wo_h, wo), (w1_h, w1), (w2_h, w2))

    def weight_copy(l, j):
        dst = pairs[j][1].at[l]
        if j == 1:
            dst = wo.at[l, pl.ds(pl.multiple_of(me * width, width), width)]
        return pltpu.make_async_copy(pairs[j][0].at[l], dst, wsem.at[l, j])

    fetches = [
        pltpu.make_async_copy(src, dst, small.at[j])
        for j, (src, dst) in enumerate(
            (
                (x_h, x_ref), (time_h, time_ref), (cond_h, cond_ref), (g1_h, g1), (b1_h, b1),
                (qkvb_h, qkvb), (ob_h, ob), (g2_h, g2), (b2_h, b2), (f1b_h, f1b), (f2b_h, f2b),
            )
        )
    ]
    for copy in fetches:
        copy.start()

    def remote(src, dst, s, r, to):
        return pltpu.make_async_remote_copy(
            src_ref=src, dst_ref=dst, send_sem=s, recv_sem=r, device_id=to, device_id_type=MESH
        )

    barrier = pltpu.get_barrier_semaphore()

    def hello(g, j):
        pl.semaphore_signal(barrier, inc=1, device_id=(g, j), device_id_type=MESH)

    for other in (partner, across, diagonal):
        hello(t, other)
    for d in range(1, groups):
        hello((t + d) % groups, me)
    for s in range(2):
        g = group_of(2 * me + s)
        j = x * 2 + (t // half + g // half) % 2

        @pl.when(jnp.logical_or(g != t, j != me))
        def _():
            hello(g, j)

    for l in range(LAYERS):
        for j in ((1, 0, 2, 3) if l == 0 else (0, 1, 2, 3)):
            weight_copy(l, j).start()
    fetches[0].wait()
    for g in range(groups):
        blk_s[g] = x_ref[g * piece : g * piece + patch]
        cnd_s[g] = x_ref[g * piece + patch : (g + 1) * piece]

    home = c == 0
    own_copies = [
        pltpu.make_async_copy(src.at[clip], dst.at[t % half], loc.at[j])
        for j, (src, dst) in enumerate(((blk_s, blk_r), (cnd_s, cnd_r)))
    ]

    @pl.when(home)
    def _():
        for copy in own_copies:
            copy.start()

    def times(axis, query):
        shape = (2 * rows, 1) if axis == 0 else (1, 2 * rows)
        at = lax.broadcasted_iota(jnp.int32, shape, axis)
        out = jnp.full(shape, FAR // 2 if query else FAR, jnp.int32)
        for f in range(groups):
            base = (f // half) * rows
            lo = base + lead + (f % half) * patch
            out = jnp.where((at >= lo) & (at < lo + patch), time_ref[:, f : f + 1], out)
            lo = base + COND * (f % half)
            hi = lo + (COND if query else cond_ref[:, f : f + 1])
            out = jnp.where((at >= lo) & (at < hi), time_ref[:, f : f + 1], out)
        return out


    targets = jnp.where(x == goal_x, half, 0)
    targets = targets - jnp.where((x == goal_x) & (goal == me) & home, 1, 0)
    with jax.named_scope("barrier"):
        pl.semaphore_wait(barrier, 3 + groups - 1 + targets)

    def enter(i, j):
        z = per * mine + (t // 2 + x) % 2
        g = 2 * z + (i + t) % 2
        k = t % half
        src, dst = ((blk_s, blk_r), (cnd_s, cnd_r))[j]
        return g, remote(src.at[clip_of(g)], dst.at[k], in_s.at[j, i], in_r.at[j, k], (g, me))

    for j in range(2):
        for i in range(2):
            g, copy = enter(i, j)

            @pl.when(g != t)
            def _():
                copy.start()

    def span(j, first, count):
        return pl.ds(pl.multiple_of(j * width + first, share), count)

    def wo_own(l):
        at = wo.at[l, span(me, 0, width)]
        return remote(at, at, ws.at[l, OWN], wr.at[l, OWN], (t, partner))

    def wo_piece(l):
        at = wo.at[l, span(me, share * t, share)]
        return remote(at, at, ws.at[l, PIECE], wr.at[l, PIECE], (t, across))

    def wo_slice(l, g):
        return wo.at[l, span(across, share * g, share)]

    def wo_column(l, d, g):
        at = wo_slice(l, g)
        to = (t + 2 * d) % groups
        return remote(at, at, ws.at[l, SPREAD + d], wr.at[l, SPREAD + d], (to, me))

    def wo_row(l, d, g):
        at = wo_slice(l, g)
        j = SPREAD + half + d
        return remote(at, at, ws.at[l, j], wr.at[l, j], (beside, me))

    def wo_rest(l):
        at = wo.at[l, span(across, 0, width)]
        return remote(at, at, ws.at[l, REST], wr.at[l, REST], (t, partner))

    def mlp_weights(l):
        return [
            remote(src.at[l], dst.at[l], ws.at[l, j], wr.at[l, j], (t, partner))
            for j, src, dst in ((UP, w1_h, w1p), (DOWN, w2_h, w2p))
        ]

    def wo_begin(l):
        weight_copy(l, 1).wait()
        wo_piece(l).start()
        wo_own(l).start()

    def wo_share(l):
        wo_piece(l).wait_recv()
        for d in range(1, half):
            wo_column(l, d, t).start()
        wo_row(l, 0, t).start()

    def wo_relay(l, d):
        g = (t - 2 * d + groups) % groups
        wo_column(l, d, g).wait_recv()
        wo_row(l, d, g).start()

    def wo_finish(l):
        for d in range(half):
            wo_row(l, d, (beside - 2 * d + groups) % groups).wait_recv()
        wo_rest(l).start()

    for copy in fetches[1:]:
        copy.wait()
    bias_copy = remote(f1b, f1p, bs.at[0], br.at[0], (t, partner))
    wo_begin(0)
    bias_copy.start()
    for copy in mlp_weights(0):
        copy.start()

    mask[...] = jnp.where(times(1, False) <= times(0, True), 0.0, -1e30)
    xs[0:lead] = jnp.zeros((lead, D), jnp.float32)

    def onward(k, j=0):
        at = (blk_r, cnd_r)[j].at[k]
        return remote(at, at, fw_s.at[j, k], fw_r.at[j, k], (t, across))

    def arrival(k, j=0):
        src, dst = ((blk_s, blk_r), (cnd_s, cnd_r))[j]
        return remote(src.at[0], dst.at[k], in_s.at[j, 0], in_r.at[j, k], (t, across))

    first_k = per * ((t // 2 + x) % 2)
    def near(i):
        return first_k + (i + t) % 2

    def cross(i):
        return per - first_k + (i + t) % 2

    for i in range(per):
        k = near(i)

        @pl.when(half * mine + k != t)
        def _():
            with jax.named_scope("in_direct"):
                arrival(k).wait_recv()
            onward(k).start()

        if i == 0:
            with jax.named_scope("wo_first"):
                wo_share(0)

    def norm(v, gain, bias):
        return layer_norm(v, gain, bias).astype(jnp.bfloat16)

    def in_half(h, r0, count):
        return pl.ds(pl.multiple_of(h * rows + r0, 16), count)

    def ids(l, kind, i):
        return ls.at[l, kind * (half + 1) + i], lr.at[l, kind * (half + 1) + i]

    def normed_send(l, i):
        at = nrm1.at[l, mine, pl.ds(*chunks[i])]
        return remote(at, at, *ids(l, N1, i), (t, partner))

    def normed_come(l, i):
        at = nrm1.at[l, 1 - mine, pl.ds(*chunks[i])]
        return remote(at, at, *ids(l, N1, i), (t, partner))

    def att_send(l, i, kind):
        at = pl.ds(*spans[i])
        to = {AP: partner, AD: diagonal, AO: across}[kind]
        src = att.at[l, me, at] if kind == AO else att_p.at[l, at]
        return remote(src, att.at[l, me, at], *ids(l, kind, i), (t, to))

    def att_come(l, i, kind):
        to = {AP: partner, AD: diagonal, AO: across}[kind]
        dst = att.at[l, to, pl.ds(*spans[i])]
        return remote(dst, dst, *ids(l, kind, i), (t, to))

    def cross_send(l, i):
        at = pl.ds(*chunks[i])
        return remote(us.at[l, at], ur.at[l, at], *ids(l, XS, i), (t, across))

    def leave(k, j=0):
        src, dst = ((out_s, out_r), (ocn_s, ocn_r))[j]
        s = clip % 2
        return remote(src.at[k], dst.at[s], os.at[j, k], orr.at[j, s], (half * mine + k, goal))

    def stay(k, j=0):
        src, dst = ((out_s, out_r), (ocn_s, ocn_r))[j]
        return pltpu.make_async_copy(src.at[k], dst.at[clip % 2], orr.at[j, clip % 2])

    def depart(k, j=0):
        here = (half * mine + k == t) & (goal == me)

        @pl.when(here)
        def _():
            stay(k, j).start()

        @pl.when(jnp.logical_not(here))
        def _():
            leave(k, j).start()

    def project(l, h, r0, m):
        at = pl.ds(r0 if isinstance(r0, int) else pl.multiple_of(r0, 16), m)
        normed = nrm1[l, h, at]
        for j, dst in enumerate((qb, kb, vb)):
            y = jnp.dot(normed, wqkv[l, j], preferred_element_type=jnp.float32)
            y = y + qkvb[j, pl.ds(l, 1)]
            if j == 0:
                y = y * head_dim ** (-0.5)
            dst[in_half(h, r0, m)] = y.astype(jnp.bfloat16)

    def strip(i):
        return pl.ds(pl.multiple_of(lead + i * patch, 16), patch) if i is not None else pl.ds(0, lead)

    def block_send(h, i):
        at = nrm1.at[0, h, strip(i)]
        return remote(at, at, *ids(0, N1, half if i is None else i), (t, partner))

    def normed_in(i):
        at = strip(i)
        nrm1[0, mine, at] = norm(xs[at], g1[0:1], b1[0:1])
        block_send(mine, i).start()

    def take(k):
        xs[strip(k)] = blk_r[k].astype(jnp.float32)
        normed_in(k)
        project(0, mine, lead + k * patch, patch)

    def take_other(k):
        with jax.named_scope("n1_wait"):
            block_send(1 - mine, k).wait_recv()
        project(0, 1 - mine, lead + k * patch, patch)

    def local(k):
        @pl.when(half * mine + k == t)
        def _():
            own_copies[0].wait()

    def relay(d):
        with jax.named_scope("wo_relay"):
            wo_relay(0, d)

    weight_copy(0, 0).wait()
    for i in range(per):
        local(near(i))
        take(near(i))
    relay(1)
    for i in range(per):
        k = cross(i)
        local(k)

        @pl.when(half * mine + k != t)
        def _():
            with jax.named_scope("in_cross"):
                onward(k).wait_recv()

        take(k)
        if i == 0:
            for j in range(per):
                k = near(j)

                @pl.when(half * mine + k != t)
                def _():
                    arrival(k, 1).wait_recv()
                    onward(k, 1).start()

        take_other(near(i))
    for d in range(2, half):
        relay(d)
    for i in range(per):
        k = cross(i)

        @pl.when(half * mine + k != t)
        def _():
            onward(k, 1).wait_recv()

    @pl.when(home)
    def _():
        own_copies[1].wait()

    for k in range(half):
        xs[COND * k : COND * (k + 1)] = cnd_r[k].astype(jnp.float32)
    normed_in(None)
    for l in range(1, LAYERS):
        wo_begin(l)
    project(0, mine, 0, lead)
    for i in range(per):
        take_other(cross(i))
    block_send(1 - mine, None).wait_recv()
    project(0, 1 - mine, 0, lead)

    lane = lax.broadcasted_iota(jnp.int32, (1, width), 1)
    heads = [(lane >= h * head_dim) & (lane < (h + 1) * head_dim) for h in range(head_local)]

    def layer(l, carry):
        def attend(h, r0, m):
            q = qb[in_half(h, r0, m)]
            stacked = jnp.concatenate(
                [q * jnp.where(on, 1.0, 0.0).astype(jnp.bfloat16) for on in heads], axis=0
            )
            sc = lax.dot_general(
                stacked, kb[...], (((1,), (1,)), ((), ())), preferred_element_type=jnp.float32
            )
            hide = mask[in_half(h, r0, m)]
            parts, totals = [], []
            for j in range(head_local):
                s = sc[j * m : (j + 1) * m] + hide
                w = jnp.exp(s - jnp.max(s, axis=-1, keepdims=True))
                totals.append(jnp.sum(w, axis=-1, keepdims=True))
                parts.append(w.astype(jnp.bfloat16))
            pv = jnp.dot(
                jnp.concatenate(parts, axis=0), vb[...], preferred_element_type=jnp.float32
            )
            acc = jnp.zeros((m, width), jnp.float32)
            for j in range(head_local):
                acc = jnp.where(heads[j], pv[j * m : (j + 1) * m] * (1.0 / totals[j]), acc)
            return acc.astype(jnp.bfloat16)

        for i, (r0, m) in enumerate(spans):
            with jax.named_scope("attend_other"):
                att_p[l, r0 : r0 + m] = attend(1 - mine, r0, m)
            att_send(l, i, AD).start()
            att_send(l, i, AP).start()
            with jax.named_scope("attend_own"):
                att[l, me, r0 : r0 + m] = attend(mine, r0, m)
            att_send(l, i, AO).start()
            if i == per - 1:
                with jax.named_scope("wo_finish"):
                    wo_finish(l)

        @pl.when(l < last)
        def _():
            for copy in mlp_weights(l + 1):
                copy.start()

        with jax.named_scope("wo_rest_wait"):
            wo_own(l).wait_recv()
            wo_rest(l).wait_recv()
        weight_copy(l, 2).wait()
        weight_copy(l, 3).wait()

        def ready(i, r0, m):
            with jax.named_scope("att_wait"):
                for kind in (AP, AD, AO):
                    att_come(l, i, kind).wait_recv()
            full = jnp.concatenate([att[l, j, r0 : r0 + m] for j in range(4)], axis=1)
            first = jnp.dot(full, wo[l], preferred_element_type=jnp.float32)
            first = xs[r0 : r0 + m] + first + ob[pl.ds(l, 1)]
            xs[r0 : r0 + m] = first
            nrm2[0:m] = norm(first, g2[pl.ds(l, 1)], b2[pl.ds(l, 1)])

        def mlp(m):
            tile = 256
            hidden = w1.shape[2]
            total = 0.0
            for p, (up, bias, down) in enumerate(((w1, f1b, w2), (w1p, f1p, w2p))):
                for n in range(hidden // tile):
                    at = pl.ds(n * tile, tile)
                    y = jnp.dot(nrm2[0:m], up[l, :, at], preferred_element_type=jnp.float32)
                    y = y + bias[pl.ds(l, 1), at]
                    y = 0.5 * y * (1.0 + lax.erf(y * (0.5**0.5)))
                    inner[0:m, pl.ds(n * tile, tile)] = y.astype(jnp.bfloat16)
                total = total + jnp.dot(
                    inner[0:m], down[l], preferred_element_type=jnp.float32
                )
            return total

        sends_x = jnp.logical_or(l < last, x != goal_x)
        takes_x = jnp.logical_or(l < last, x == goal_x)

        for i, (r0, m) in enumerate(spans):
            ready(i, r0, m)
            if i == 0:
                with jax.named_scope("weights_wait"):

                    @pl.when(l == 0)
                    def _():
                        bias_copy.wait_recv()

                    for copy in mlp_weights(l):
                        copy.wait_recv()
            with jax.named_scope("mlp"):
                u = mlp(m)
                keep[r0 : r0 + m] = u
                us[l, r0 : r0 + m] = u.astype(jnp.bfloat16)

            @pl.when(sends_x)
            def _():
                for j in members[i]:
                    cross_send(l, j).start()

            if i == 0:

                @pl.when(l < last)
                def _():
                    wo_share(l + 1)

        @pl.when(l < last)
        def _():
            weight_copy(l + 1, 0).wait()

        def other(i):
            with jax.named_scope("n1_wait"):
                normed_come(l + 1, i).wait_recv()
            project(l + 1, 1 - mine, *chunks[i])

        for i, (r0, m) in enumerate(chunks):

            @pl.when(takes_x)
            def _():
                with jax.named_scope("x_wait"):
                    cross_send(l, i).wait_recv()
                new = xs[r0 : r0 + m] + keep[r0 : r0 + m] + f2b[pl.ds(l, 1)]
                new = (new + ur[l, r0 : r0 + m].astype(jnp.float32)).astype(jnp.bfloat16)

                @pl.when(l < last)
                def _():
                    wide = new.astype(jnp.float32)
                    xs[r0 : r0 + m] = wide
                    nrm1[l + 1, mine, r0 : r0 + m] = norm(
                        wide, g1[pl.ds(l + 1, 1)], b1[pl.ds(l + 1, 1)]
                    )
                    normed_send(l + 1, i).start()
                    project(l + 1, mine, r0, m)
                    if i > 0:
                        other(i - 1)

                @pl.when(l == last)
                def _():
                    out_s[i] = new[m - patch :]
                    depart(i)
                    if i == 0:
                        for k in range(half):
                            ocn_s[k] = new[COND * k : COND * (k + 1)]
                            depart(k, 1)

            if i == half - 3:

                @pl.when(l < last)
                def _():
                    with jax.named_scope("wo_relay"):
                        for d in range(1, half):
                            wo_relay(l + 1, d)

        @pl.when(l < last)
        def _():
            other(half - 1)

        return carry

    lax.fori_loop(0, LAYERS, layer, 0)

    for i in range(2):
        for j in range(2):
            g, copy = enter(i, j)

            @pl.when(g != t)
            def _():
                copy.wait_send()

    for i in range(per):
        k = near(i)

        @pl.when(half * mine + k != t)
        def _():
            for j in range(2):
                onward(k, j).wait_send()

    bias_copy.wait_send()
    for i in range(half):
        block_send(mine, i).wait_send()
    block_send(mine, None).wait_send()

    def drain(l, carry):
        for i in range(half):

            @pl.when(l > 0)
            def _():
                normed_send(l, i).wait_send()

            @pl.when(jnp.logical_or(l < last, x != goal_x))
            def _():
                cross_send(l, i).wait_send()

        for i in range(len(spans)):
            for kind in (AP, AD, AO):
                att_send(l, i, kind).wait_send()

        wo_own(l).wait_send()
        wo_piece(l).wait_send()
        wo_rest(l).wait_send()
        for d in range(1, half):
            wo_column(l, d, t).wait_send()
        for d in range(half):
            wo_row(l, d, t).wait_send()
        for copy in mlp_weights(l):
            copy.wait_send()
        return carry

    lax.fori_loop(0, LAYERS, drain, 0)

    for s in range(2):
        there = 2 * me + s
        here = (group_of(there) == t) & home

        @pl.when(here)
        def _():
            for j, (src, dst) in enumerate(((out_s, out_r), (ocn_s, ocn_r))):
                pltpu.make_async_copy(src.at[t % half], dst.at[s], orr.at[j, s]).wait()

        @pl.when(jnp.logical_not(here))
        def _():
            with jax.named_scope("out_wait"):
                for j, (src, dst) in enumerate(((out_s, out_r), (ocn_s, ocn_r))):
                    remote(
                        src.at[0], dst.at[s], os.at[j, 0], orr.at[j, s], (t, across)
                    ).wait_recv()

        out_ref[s * piece : s * piece + patch] = out_r[s]
        out_ref[s * piece + patch : (s + 1) * piece] = ocn_r[s]

    for k in range(half):
        here = (half * mine + k == t) & (goal == me)

        @pl.when((x == goal_x) & jnp.logical_not(here))
        def _():
            for j in range(2):
                leave(k, j).wait_send()


def shards_clip(
    frames_in,
    frame_time,
    cond_count,
    ln1_gain,
    ln1_bias,
    qkv_weight,
    qkv_bias,
    out_weight,
    out_bias,
    ln2_gain,
    ln2_bias,
    fc1_weight,
    fc1_bias,
    fc2_weight,
    fc2_bias,
):
    groups = lax.axis_size("tm")
    tensor_size = lax.axis_size("tensor")
    piece = PATCH_DEV + COND
    half = groups // 2
    width = qkv_weight.shape[3]
    hidden = fc1_weight.shape[2]
    lead = -(-half * COND // 16) * 16
    rows = lead + half * PATCH_DEV
    chunk = lead + (half - half // 2) * PATCH_DEV

    vmem = pl.BlockSpec(memory_space=pltpu.VMEM)
    hbm = pl.BlockSpec(memory_space=pl.ANY)
    bf16, f32 = jnp.bfloat16, jnp.float32
    dma = pltpu.SemaphoreType.DMA
    out = pl.pallas_call(
        clip_kernel,
        out_shape=jax.ShapeDtypeStruct((2 * piece, D), bf16),
        in_specs=[hbm] * 15,
        out_specs=vmem,
        scratch_shapes=[
            pltpu.VMEM(frames_in.shape[1:], bf16),
            pltpu.VMEM((1, groups), jnp.int32),
            pltpu.VMEM((1, groups), jnp.int32),
            pltpu.VMEM(ln1_gain.shape, f32),
            pltpu.VMEM(ln1_bias.shape, f32),
            pltpu.VMEM((3, LAYERS, width), f32),
            pltpu.VMEM(out_bias.shape, f32),
            pltpu.VMEM(ln2_gain.shape, f32),
            pltpu.VMEM(ln2_bias.shape, f32),
            pltpu.VMEM(fc1_bias.shape, f32),
            pltpu.VMEM(fc2_bias.shape, f32),
            dma((11,)),
            pltpu.VMEM(qkv_weight.shape, bf16),
            pltpu.VMEM((LAYERS, D, D), bf16),
            pltpu.VMEM(fc1_weight.shape, bf16),
            pltpu.VMEM(fc2_weight.shape, bf16),
            pltpu.VMEM(fc1_weight.shape, bf16),
            pltpu.VMEM(fc2_weight.shape, bf16),
            pltpu.VMEM(fc1_bias.shape, f32),
            pltpu.VMEM((groups, PATCH_DEV, D), bf16),
            pltpu.VMEM((groups, COND, D), bf16),
            pltpu.VMEM((half, PATCH_DEV, D), bf16),
            pltpu.VMEM((half, COND, D), bf16),
            pltpu.VMEM((rows, D), f32),
            pltpu.VMEM((rows, D), f32),
            pltpu.VMEM((LAYERS, 2, rows, D), bf16),
            pltpu.VMEM((chunk, D), bf16),
            pltpu.VMEM((2 * rows, width), bf16),
            pltpu.VMEM((2 * rows, width), bf16),
            pltpu.VMEM((2 * rows, width), bf16),
            pltpu.VMEM((2 * rows, 2 * rows), f32),
            pltpu.VMEM((LAYERS, tensor_size, rows, width), bf16),
            pltpu.VMEM((LAYERS, rows, width), bf16),
            pltpu.VMEM((chunk, hidden), bf16),
            pltpu.VMEM((LAYERS, rows, D), bf16),
            pltpu.VMEM((LAYERS, rows, D), bf16),
            pltpu.VMEM((half, PATCH_DEV, D), bf16),
            pltpu.VMEM((2, PATCH_DEV, D), bf16),
            pltpu.VMEM((half, COND, D), bf16),
            pltpu.VMEM((2, COND, D), bf16),
            dma((LAYERS, 4)),
            dma((2, half)),
            dma((2, half)),
            dma((2, half)),
            dma((2, half)),
            dma((2,)),
            dma((1,)),
            dma((1,)),
            dma((LAYERS, 5 * (half + 1))),
            dma((LAYERS, 5 * (half + 1))),
            dma((LAYERS, SPREAD + 2 * half)),
            dma((LAYERS, SPREAD + 2 * half)),
            dma((2, half)),
            dma((2, 2)),
        ],
        compiler_params=pltpu.CompilerParams(
            collective_id=0, has_side_effects=True, vmem_limit_bytes=60 * 1024 * 1024
        ),
    )(
        frames_in[0],
        frame_time.reshape(1, groups),
        cond_count.reshape(1, groups),
        ln1_gain,
        ln1_bias,
        qkv_bias.transpose(1, 0, 2),
        out_bias,
        ln2_gain,
        ln2_bias,
        fc1_bias,
        fc2_bias,
        qkv_weight,
        out_weight,
        fc1_weight,
        fc2_weight,
    )
    return out[None]


def shards(frames_in, frame_time, cond_count, *rest):
    groups = lax.axis_size("tm")
    seq_count = frames_in.shape[1] // (PATCH_DEV + COND)
    by_clip = frame_time.shape[0] == groups and seq_count == groups
    by_clip = by_clip and lax.axis_size("tensor") == 4 and groups == 8
    body = shards_clip if by_clip else shards_gather
    return body(frames_in, frame_time, cond_count, *rest)


def solution(mesh):
    in_specs = (
        P("tm", None, None),
        P(),
        P(),
        P(),
        P(),
        P(None, None, None, "tensor"),
        P(None, None, "tensor"),
        P(None, "tensor", None),
        P(),
        P(),
        P(),
        P(None, None, "tensor"),
        P(None, "tensor"),
        P(None, "tensor", None),
        P(),
    )
    out_specs = P("tm", "tensor", None)
    return jax.shard_map(shards, mesh=mesh, in_specs=in_specs, out_specs=out_specs, check_vma=False)
```
